32 devices in a mesh: dp: 1 (over z), tp: 4 (over y), sp: 8 (over x, core).
Axes of the slice: x: 4, y: 4, z: 1, core: 2. Of those that a mesh axis runs over, the one named last changes fastest.
The devices are a block of a 4x4x8 slice.
Arguments:
- x_in: bfloat16 [128, 5376], P('dp')
- cur_pos: int32 [128], P('dp')
- w_pre: float32 [5376], replicated
- w_q: bfloat16 [5376, 4096], P(None, 'tp')
- w_k: bfloat16 [5376, 2048], P(None, 'tp')
- w_v: bfloat16 [5376, 2048], P(None, 'tp')
- w_o: bfloat16 [4096, 5376], P('tp')
- w_post: float32 [5376], replicated
- k_cache: bfloat16 [128, 512, 16, 128], P('dp', 'sp', 'tp')
- v_cache: bfloat16 [128, 512, 16, 128], P('dp', 'sp', 'tp')
Outputs:
- output 1: bfloat16 [128, 5376], P('dp')
- output 2: bfloat16 [128, 512, 16, 128], P('dp', 'sp', 'tp')
- output 3: bfloat16 [128, 512, 16, 128], P('dp', 'sp', 'tp')
All inputs are finite; a program needn't handle non-finite values.
Results may differ from the reference program's by a relative error of at most 0.00624945.
Values sent between devices are 32-bit elements.
A program may use at most 768 MiB of HBM per device.

```python
import jax
import jax.numpy as jnp
from jax import lax

BATCH_SIZE = 128
SEQ_LEN = 512
D_MODEL = 5376
NUM_HEADS = 32
KV_HEADS = 16
HEAD_DIM = 128
HOT_KEYS = 48

SOFT_CAP = 50.0
ROPE_BASE = 10000.0
NORM_EPS = 1e-6


def rms_scale(tensor, gain_w):
    mean_sq = jnp.mean(tensor * tensor, axis=-1, keepdims=True)
    return tensor * lax.rsqrt(mean_sq + NORM_EPS) * (1.0 + gain_w)


def rotary(tensor, positions):
    half_dim = tensor.shape[-1] // 2
    inv_freq = ROPE_BASE ** (-2.0 * jnp.arange(half_dim, dtype=jnp.float32) / (2 * half_dim))
    angles = positions.astype(jnp.float32)[:, None] * inv_freq[None, :]
    angles = angles.reshape((angles.shape[0],) + (1,) * (tensor.ndim - 2) + (half_dim,))
    cos_tab = jnp.cos(angles)
    sin_tab = jnp.sin(angles)
    lo_half = tensor[..., :half_dim]
    hi_half = tensor[..., half_dim:]
    return jnp.concatenate([lo_half * cos_tab - hi_half * sin_tab, hi_half * cos_tab + lo_half * sin_tab], axis=-1)


def setup_inputs(seed: int = 0, part: int = 0) -> dict:
    part_keys = jax.random.split(jax.random.fold_in(jax.random.key(seed), part), 6)
    shared_keys = jax.random.split(jax.random.key(seed + 1), 7)
    q_cols = NUM_HEADS * HEAD_DIM
    kv_cols = KV_HEADS * HEAD_DIM
    cache_shape = (BATCH_SIZE, SEQ_LEN, KV_HEADS, HEAD_DIM)
    x_in = jax.random.normal(part_keys[0], (BATCH_SIZE, D_MODEL), jnp.float32).astype(jnp.bfloat16)
    drawn_pos = jax.random.randint(part_keys[1], (BATCH_SIZE,), 0, SEQ_LEN)
    long_row = jax.random.randint(part_keys[2], (), 0, BATCH_SIZE)
    cur_pos = jnp.where(jnp.arange(BATCH_SIZE) == long_row, SEQ_LEN - 1, drawn_pos).astype(jnp.int32)
    hot_mark = jax.random.randint(part_keys[3], (BATCH_SIZE, SEQ_LEN, KV_HEADS, 1), 0, SEQ_LEN) < HOT_KEYS
    key_scale = jnp.where(hot_mark, 2.5, 0.03)
    k_cache = (jax.random.normal(part_keys[4], cache_shape, jnp.float32) * key_scale).astype(jnp.bfloat16)
    v_cache = jax.random.normal(part_keys[5], cache_shape, jnp.float32).astype(jnp.bfloat16)
    w_pre = 0.5 * jax.random.normal(shared_keys[0], (D_MODEL,), jnp.float32)
    w_q = (jax.random.normal(shared_keys[1], (D_MODEL, q_cols), jnp.float32) * (36.0 * D_MODEL ** -0.5)).astype(jnp.bfloat16)
    w_k = (jax.random.normal(shared_keys[2], (D_MODEL, kv_cols), jnp.float32) * (2.2 * D_MODEL ** -0.5)).astype(jnp.bfloat16)
    w_v = (jax.random.normal(shared_keys[3], (D_MODEL, kv_cols), jnp.float32) * D_MODEL ** -0.5).astype(jnp.bfloat16)
    w_o = (jax.random.normal(shared_keys[4], (q_cols, D_MODEL), jnp.float32) * q_cols ** -0.5).astype(jnp.bfloat16)
    w_post = 0.5 * jax.random.normal(shared_keys[5], (D_MODEL,), jnp.float32)
    return {'x_in': x_in, 'cur_pos': cur_pos, 'w_pre': w_pre, 'w_q': w_q, 'w_k': w_k, 'w_v': w_v, 'w_o': w_o, 'w_post': w_post, 'k_cache': k_cache, 'v_cache': v_cache}


def reference(x_in, cur_pos, w_pre, w_q, w_k, w_v, w_o, w_post, k_cache, v_cache):
    group_size = NUM_HEADS // KV_HEADS
    seq_ids = jnp.arange(SEQ_LEN)
    normed = rms_scale(x_in.astype(jnp.float32), w_pre).astype(jnp.bfloat16)
    q_proj = jnp.dot(normed, w_q, preferred_element_type=jnp.float32).reshape(BATCH_SIZE, NUM_HEADS, HEAD_DIM)
    k_proj = jnp.dot(normed, w_k, preferred_element_type=jnp.float32).reshape(BATCH_SIZE, KV_HEADS, HEAD_DIM)
    q_rot = rotary(q_proj, cur_pos).astype(jnp.bfloat16)
    k_new = rotary(k_proj, cur_pos).astype(jnp.bfloat16)
    v_new = jnp.dot(normed, w_v, preferred_element_type=jnp.float32).reshape(BATCH_SIZE, KV_HEADS, HEAD_DIM).astype(jnp.bfloat16)
    slot_hit = (seq_ids[None, :] == cur_pos[:, None])[:, :, None, None]
    k_out = jnp.where(slot_hit, k_new[:, None], k_cache)
    v_out = jnp.where(slot_hit, v_new[:, None], v_cache)

    def one_row(row_data):
        q_row, k_row, v_row, pos_row = row_data
        q_grp = q_row.astype(jnp.float32).reshape(KV_HEADS, group_size, HEAD_DIM)
        raw_score = jnp.einsum('grd,tgd->grt', q_grp, k_row.astype(jnp.float32)) * HEAD_DIM ** -0.5
        capped = SOFT_CAP * jnp.tanh(raw_score / SOFT_CAP)
        capped = jnp.where(seq_ids <= pos_row, capped, -jnp.inf)
        prob_w = jax.nn.softmax(capped, axis=-1)
        attn_row = jnp.einsum('grt,tgd->grd', prob_w, v_row.astype(jnp.float32))
        return attn_row.reshape(NUM_HEADS * HEAD_DIM)

    attn_out = lax.map(one_row, (q_rot, k_out, v_out, cur_pos))
    proj_sum = jnp.dot(attn_out.astype(jnp.bfloat16), w_o, preferred_element_type=jnp.float32)
    x_out = (x_in.astype(jnp.float32) + rms_scale(proj_sum, w_post)).astype(jnp.bfloat16)
    return (x_out, k_out, v_out)
```

```python
import functools

import jax
import jax.numpy as jnp
from jax import lax
from jax.experimental import pallas as pl
from jax.experimental.pallas import tpu as pltpu
from jax.sharding import PartitionSpec as P

SOFT_CAP = 50.0
ROPE_BASE = 10000.0
NORM_EPS = 1e-6
NEG_FILL = -1e30
MESH = pl.DeviceIdType.MESH
RING = 4


def rms_scale(tensor, gain_w):
    mean_sq = jnp.mean(tensor * tensor, axis=-1, keepdims=True)
    return tensor * lax.rsqrt(mean_sq + NORM_EPS) * (1.0 + gain_w)


def rotary(tensor, positions):
    half_dim = tensor.shape[-1] // 2
    inv_freq = ROPE_BASE ** (-2.0 * jnp.arange(half_dim, dtype=jnp.float32) / (2 * half_dim))
    angles = positions.astype(jnp.float32)[:, None] * inv_freq[None, :]
    angles = angles.reshape((angles.shape[0],) + (1,) * (tensor.ndim - 2) + (half_dim,))
    cos_tab = jnp.cos(angles)
    sin_tab = jnp.sin(angles)
    lo_half = tensor[..., :half_dim]
    hi_half = tensor[..., half_dim:]
    return jnp.concatenate([lo_half * cos_tab - hi_half * sin_tab, hi_half * cos_tab + lo_half * sin_tab], axis=-1)


FIRST_P, FIRST_M, DIAG_A, DIAG_B = 0, 1, 2, 3
UNITS = ('own', 'prev', 'next', 'diag_a', 'diag_b')
SECOND = {(u, d): 4 + 2 * i + j for i, u in enumerate(UNITS) for j, d in enumerate((1, -1))}
FORWARD = {u: 14 + i for i, u in enumerate(('own_a', 'own_b', 'prev', 'next', 'diag_a', 'diag_b'))}
N_GATHER = 20


def comm_kernel(heads, o_ref, wo_hbm, x_hbm, wpost_ref, out_ref,
                wo_v, x_v, pair_r, comb, sp_r, scr, part, tp_r, gath,
                wo_sem, x_sem, pair_ss, pair_rs, sp_ss, sp_rs, tp_ss, tp_rs, ag_ss, ag_rs, dd_ss, dd_rs):
    y = lax.axis_index('tp')
    s = lax.axis_index('sp')
    xc = s // 2
    c = s % 2
    slab_rows, dim = comb.shape[1], comb.shape[2]
    row_block = (slab_rows - 2 * heads) // heads
    sub = row_block // RING
    width = part.shape[2]
    stat = row_block * heads

    def chip(dx, dy):
        return {'tp': (y + dy) % RING, 'sp': ((xc + dx) % RING) * 2 + c}

    partner = {'sp': xc * 2 + (1 - c)}

    barrier = pltpu.get_barrier_semaphore()
    pl.semaphore_signal(barrier, inc=1, device_id=partner, device_id_type=MESH)
    for k in range(1, RING):
        pl.semaphore_signal(barrier, inc=1, device_id=chip(k, 0), device_id_type=MESH)
        pl.semaphore_signal(barrier, inc=1, device_id=chip(0, k), device_id_type=MESH)

    wo_rows = wo_v.shape[0] // RING
    wo_copies = []
    for i in range(RING):
        rows = pl.ds(i * wo_rows, wo_rows)
        wo_copies.append(pltpu.make_async_copy(wo_hbm.at[rows], wo_v.at[rows], wo_sem.at[i]))
        wo_copies[-1].start()
    x_copy = pltpu.make_async_copy(x_hbm.at[pl.ds(pl.multiple_of(s * row_block, row_block), row_block)], x_v, x_sem)
    x_copy.start()

    pl.semaphore_wait(barrier, 2 * RING - 1)

    order = (2, 1, 3, 0)
    pair = []
    for k in order:
        there = (xc + k) % RING
        pair.append(pltpu.make_async_remote_copy(
            src_ref=o_ref.at[(1 - c) * RING + there], dst_ref=pair_r.at[there],
            send_sem=pair_ss.at[k], recv_sem=pair_rs.at[k], device_id=partner, device_id_type=MESH))
        pair[-1].start()
    sp_copies = {}
    for i, k in enumerate(order):
        there = (xc + k) % RING
        mine = c * RING + there
        pair[i].wait_recv()
        m0 = o_ref[mine, pl.ds(stat, heads), :]
        l0 = o_ref[mine, pl.ds(stat + heads, heads), :]
        m1 = pair_r[there, pl.ds(stat, heads), :]
        l1 = pair_r[there, pl.ds(stat + heads, heads), :]
        top = jnp.maximum(m0, m1)
        f0 = jnp.exp(m0 - top)
        f1 = jnp.exp(m1 - top)
        comb[there, pl.ds(stat, heads), :] = top
        comb[there, pl.ds(stat + heads, heads), :] = l0 * f0 + l1 * f1
        for j in range(row_block):
            rows = pl.ds(j * heads, heads)
            comb[there, rows, :] = o_ref[mine, rows, :] * f0[:, j:j + 1] + pair_r[there, rows, :] * f1[:, j:j + 1]
        if k:
            sp_copies[k] = pltpu.make_async_remote_copy(
                src_ref=comb.at[there], dst_ref=sp_r.at[RING - k - 1],
                send_sem=sp_ss.at[k - 1], recv_sem=sp_rs.at[RING - k - 1], device_id=chip(k, 0), device_id_type=MESH)
            sp_copies[k].start()

    def arrived(k):
        return pltpu.make_async_remote_copy(
            src_ref=comb.at[xc], dst_ref=sp_r.at[k - 1], send_sem=sp_ss.at[k - 1], recv_sem=sp_rs.at[k - 1],
            device_id=chip(k, 0), device_id_type=MESH)
    for k in (1, 3, 2):
        arrived(k).wait_recv()
    m_all = [comb[xc, pl.ds(stat, heads), :]] + [sp_r[k, pl.ds(stat, heads), :] for k in range(RING - 1)]
    l_all = [comb[xc, pl.ds(stat + heads, heads), :]] + [sp_r[k, pl.ds(stat + heads, heads), :] for k in range(RING - 1)]
    top = functools.reduce(jnp.maximum, m_all)
    f_all = [jnp.exp(m - top) for m in m_all]
    total = sum(l * f for l, f in zip(l_all, f_all))
    lane = lax.broadcasted_iota(jnp.int32, total.shape, 1)
    inv = 1.0 / jnp.where(lane < row_block, total, 1.0)
    f_all = [f * inv for f in f_all]
    for j in range(row_block):
        rows = pl.ds(j * heads, heads)
        acc = comb[xc, rows, :] * f_all[0][:, j:j + 1]
        for k in range(RING - 1):
            acc += sp_r[k, rows, :] * f_all[k + 1][:, j:j + 1]
        scr[rows, :] = acc
    attn = jnp.concatenate([scr[pl.ds(h, row_block, stride=heads), :].astype(jnp.bfloat16) for h in range(heads)], axis=1)

    for copy in wo_copies:
        copy.wait()
    n_chunk = tp_ss.shape[0] // (RING - 1)
    cols = width // n_chunk
    tp_copies = []
    for n in range(n_chunk):
        span = pl.ds(n * cols, cols)
        prod = jnp.dot(attn, wo_v[:, span], preferred_element_type=jnp.float32)
        for t in range(RING):
            part[t, :, span] = prod[t * sub:(t + 1) * sub]
        for k in (2, 1, 3):
            to = (y + k) % RING
            copy = pltpu.make_async_remote_copy(
                src_ref=part.at[to, :, span], dst_ref=tp_r.at[RING - k - 1, :, span],
                send_sem=tp_ss.at[n * (RING - 1) + k - 1], recv_sem=tp_rs.at[n * (RING - 1) + RING - k - 1],
                device_id=chip(0, k), device_id_type=MESH)
            copy.start()
            tp_copies.append(copy)
    x_copy.wait()
    for copy in tp_copies:
        copy.wait_recv()
    ssq = jnp.zeros((sub, 1), jnp.float32)
    u_all = []
    for n in range(n_chunk):
        span = pl.ds(n * cols, cols)
        u = part[y, :, span]
        for k in range(RING - 1):
            u += tp_r[k, :, span]
        ssq += jnp.sum(u * u, axis=1, keepdims=True)
        u_all.append(u)
    scale = lax.rsqrt(ssq / width + NORM_EPS)

    a, b = xc * (1 - c) + y * c, y * (1 - c) + xc * c

    def place(da, db):
        return c * RING * RING + ((a + da) % RING) * RING + (b + db) % RING

    for n in range(n_chunk):
        span = pl.ds(n * cols, cols)
        x16 = x_v[:, span].astype(jnp.float32)
        x4 = x16[0:sub]
        for t in range(1, RING):
            x4 = jnp.where(y == t, x16[t * sub:(t + 1) * sub], x4)
        gath[place(0, 0), :, span] = x4 + u_all[n] * scale * (1.0 + wpost_ref[:, span])

    def device(da, db):
        return chip(da * (1 - c) + db * c, db * (1 - c) + da * c)

    half = width // 2
    parts = {'': pl.ds(0, width), 'a': pl.ds(0, half), 'b': pl.ds(half, half)}

    def message(src, part_key, to, number):
        ref = gath.at[place(*src), :, parts[part_key]]
        return pltpu.make_async_remote_copy(
            src_ref=ref, dst_ref=ref, send_sem=ag_ss.at[number], recv_sem=ag_rs.at[number],
            device_id=device(*to), device_id_type=MESH)

    sent = []

    def send(*args):
        copy = message(*args)
        copy.start()
        sent.append(copy)

    def wait(src, part_key, number):
        message(src, part_key, (0, 0), number).wait_recv()

    def to_pair(da, db):
        ref = gath.at[place(da, db)]
        number = da % RING * RING + db % RING
        copy = pltpu.make_async_remote_copy(
            src_ref=ref, dst_ref=ref, send_sem=dd_ss.at[number], recv_sem=dd_rs.at[number],
            device_id=partner, device_id_type=MESH)
        copy.start()
        sent.append(copy)

    unit = {'own': (0, ''), 'prev': (-1, ''), 'next': (1, ''), 'diag_a': (2, 'a'), 'diag_b': (2, 'b')}

    def second(name):
        da, key = unit[name]
        for d in (1, -1):
            send((da, 0), key, (0, d), SECOND[name, d])

    def got_second(name, d):
        da, key = unit[name]
        wait((da, -d), key, SECOND[name, d])

    def forward(da, d, key, name):
        send((da, -d), key, (0, d), FORWARD[name])

    send((0, 0), '', (1, 0), FIRST_P)
    send((0, 0), '', (-1, 0), FIRST_M)
    second('own')
    to_pair(0, 0)
    wait((-1, 0), '', FIRST_P)
    send((-1, 0), 'a', (1, 0), DIAG_A)
    second('prev')
    to_pair(-1, 0)
    wait((1, 0), '', FIRST_M)
    send((1, 0), 'b', (-1, 0), DIAG_B)
    second('next')
    to_pair(1, 0)
    got_second('own', 1)
    forward(0, 1, 'a', 'own_a')
    to_pair(0, -1)
    got_second('own', -1)
    forward(0, -1, 'b', 'own_b')
    to_pair(0, 1)
    wait((2, 0), 'a', DIAG_A)
    second('diag_a')
    wait((2, 0), 'b', DIAG_B)
    second('diag_b')
    to_pair(2, 0)
    got_second('prev', 1)
    forward(-1, 1, '', 'prev')
    to_pair(-1, -1)
    got_second('next', -1)
    forward(1, -1, '', 'next')
    to_pair(1, 1)
    got_second('prev', -1)
    to_pair(-1, 1)
    got_second('next', 1)
    to_pair(1, -1)
    wait((0, 2), 'a', FORWARD['own_a'])
    wait((0, 2), 'b', FORWARD['own_b'])
    to_pair(0, 2)
    got_second('diag_a', 1)
    forward(2, 1, 'a', 'diag_a')
    got_second('diag_b', -1)
    forward(2, -1, 'b', 'diag_b')
    got_second('diag_b', 1)
    to_pair(2, -1)
    got_second('diag_a', -1)
    to_pair(2, 1)
    wait((-1, 2), '', FORWARD['prev'])
    to_pair(-1, 2)
    wait((1, 2), '', FORWARD['next'])
    to_pair(1, 2)
    wait((2, 2), 'a', FORWARD['diag_a'])
    wait((2, 2), 'b', FORWARD['diag_b'])
    to_pair(2, 2)

    a2, b2 = b, a
    for da in range(RING):
        for db in range(RING):
            ref = gath.at[(1 - c) * RING * RING + ((a2 + da) % RING) * RING + (b2 + db) % RING]
            pltpu.make_async_remote_copy(
                src_ref=ref, dst_ref=ref, send_sem=dd_ss.at[da * RING + db], recv_sem=dd_rs.at[da * RING + db],
                device_id=partner, device_id_type=MESH).wait_recv()

    for cx in range(RING):
        for cc in range(2):
            rows = pl.ds((2 * cx + cc) * row_block, row_block)
            for n in range(n_chunk):
                span = pl.ds(n * cols, cols)
                blocks = [gath[cx * RING + t if cc == 0 else RING * RING + t * RING + cx, :, span] for t in range(RING)]
                out_ref[rows, span] = jnp.concatenate(blocks, axis=0).astype(out_ref.dtype)

    for copy in pair:
        copy.wait_send()
    for copy in list(sp_copies.values()) + tp_copies + sent:
        copy.wait_send()


def finish(o_pack, w_o, x_in, w_post, heads):
    rows, width = x_in.shape
    _, slab_rows, dim = o_pack.shape
    row_block = rows // (2 * RING)
    n_chunk = 3 if width % (3 * 256) == 0 else 1
    sems = pltpu.SemaphoreType.DMA
    vmem = pl.BlockSpec(memory_space=pltpu.VMEM)
    return pl.pallas_call(
        functools.partial(comm_kernel, heads),
        out_shape=jax.ShapeDtypeStruct((rows, width), x_in.dtype),
        in_specs=[vmem, pl.BlockSpec(memory_space=pl.ANY), pl.BlockSpec(memory_space=pl.ANY), vmem],
        out_specs=vmem,
        scratch_shapes=[
            pltpu.VMEM(w_o.shape, w_o.dtype),
            pltpu.VMEM((row_block, width), x_in.dtype),
            pltpu.VMEM((RING, slab_rows, dim), jnp.float32),
            pltpu.VMEM((RING, slab_rows, dim), jnp.float32),
            pltpu.VMEM((RING - 1, slab_rows, dim), jnp.float32),
            pltpu.VMEM((row_block * heads, dim), jnp.float32),
            pltpu.VMEM((RING, row_block // RING, width), jnp.float32),
            pltpu.VMEM((RING - 1, row_block // RING, width), jnp.float32),
            pltpu.VMEM((2 * RING * RING, row_block // RING, width), jnp.float32),
            sems((RING,)), sems(()),
            sems((RING,)), sems((RING,)),
            sems((RING - 1,)), sems((RING - 1,)),
            sems((n_chunk * (RING - 1),)), sems((n_chunk * (RING - 1),)),
            sems((N_GATHER,)), sems((N_GATHER,)),
            sems((RING * RING,)), sems((RING * RING,)),
        ],
        compiler_params=pltpu.CompilerParams(collective_id=0, has_side_effects=True, vmem_limit_bytes=40 * 2**20),
        cost_estimate=pl.CostEstimate(flops=2 * rows * w_o.size // 8, bytes_accessed=w_o.size * 2, transcendentals=0),
        name='finish',
    )(o_pack, w_o, x_in, w_post[None])


def solution(mesh):
    cache_spec = P('dp', 'sp', 'tp', None)
    n_sp = mesh.shape['sp']
    assert n_sp == 2 * RING and mesh.shape['tp'] == RING

    def local_step(x_in, cur_pos, w_pre, w_q, w_k, w_v, w_o, w_post, k_cache, v_cache):
        row_count, seq_block, kv_local, head_dim = k_cache.shape
        heads_local = w_q.shape[1] // head_dim
        group_size = heads_local // kv_local
        sp_index = lax.axis_index('sp')
        normed = rms_scale(x_in.astype(jnp.float32), w_pre).astype(jnp.bfloat16)
        q_proj = jnp.dot(normed, w_q, preferred_element_type=jnp.float32)
        q_rot = rotary(q_proj.reshape(row_count, kv_local, group_size, head_dim), cur_pos).astype(jnp.bfloat16)
        k_proj = jnp.dot(normed, w_k, preferred_element_type=jnp.float32)
        k_new = rotary(k_proj.reshape(row_count, kv_local, head_dim), cur_pos).astype(jnp.bfloat16)
        v_new = jnp.dot(normed, w_v, preferred_element_type=jnp.float32).reshape(row_count, kv_local, head_dim).astype(jnp.bfloat16)
        block_pos = sp_index * seq_block + jnp.arange(seq_block)
        slot_hit = (block_pos[None, :] == cur_pos[:, None])[:, :, None, None]
        k_out = jnp.where(slot_hit, k_new[:, None], k_cache)
        v_out = jnp.where(slot_hit, v_new[:, None], v_cache)
        raw_score = jnp.einsum('bgrd,btgd->bgrt', q_rot, k_out, preferred_element_type=jnp.float32)
        capped = SOFT_CAP * jnp.tanh(raw_score * (head_dim ** -0.5 / SOFT_CAP))
        is_valid = (block_pos[None, :] <= cur_pos[:, None])[:, None, None, :]
        capped = jnp.where(is_valid, capped, NEG_FILL)
        block_max = jnp.max(capped, axis=-1)
        exp_w = jnp.where(is_valid, jnp.exp(capped - block_max[..., None]), 0.0)
        block_sum = jnp.sum(exp_w, axis=-1)
        block_out = jnp.einsum('bgrt,btgd->bgrd', exp_w.astype(jnp.bfloat16), v_out, preferred_element_type=jnp.float32)

        row_block = row_count // n_sp

        def stat_tile(t):
            t = t.reshape(n_sp, row_block, heads_local).transpose(0, 2, 1)
            return jnp.pad(t, ((0, 0), (0, 0), (0, head_dim - row_block)))

        slabs = jnp.concatenate([block_out.reshape(n_sp, row_block * heads_local, head_dim), stat_tile(block_max), stat_tile(block_sum)], axis=1)
        slabs = slabs.reshape(RING, 2, *slabs.shape[1:]).transpose(1, 0, 2, 3).reshape(slabs.shape)
        x_out = finish(slabs, w_o, x_in, w_post, heads_local)
        return x_out, k_out, v_out

    return jax.shard_map(local_step, mesh=mesh,
                         in_specs=(P('dp', None), P('dp'), P(None), P(None, 'tp'), P(None, 'tp'), P(None, 'tp'), P('tp', None), P(None), cache_spec, cache_spec),
                         out_specs=(P('dp', None), cache_spec, cache_spec), check_vma=False)
```

```python
import functools

import jax
import jax.numpy as jnp
from jax import lax
from jax.experimental import pallas as pl
from jax.experimental.pallas import tpu as pltpu
from jax.sharding import PartitionSpec as P

SOFT_CAP = 50.0
ROPE_BASE = 10000.0
NORM_EPS = 1e-6
NEG_FILL = -1e30
MESH = pl.DeviceIdType.MESH
RING = 4


FIRST_P, FIRST_M, DIAG_A, DIAG_B = 0, 1, 2, 3
UNITS = ('own', 'prev', 'next', 'diag_a', 'diag_b')
SECOND = {(u, d): 4 + 2 * i + j for i, u in enumerate(UNITS) for j, d in enumerate((1, -1))}
FORWARD = {u: 14 + i for i, u in enumerate(('own_a', 'own_b', 'prev', 'next', 'diag_a', 'diag_b'))}
N_GATHER = 20


def comm_kernel(heads, o_ref, wo_hbm, x_hbm, wpost_ref, out_ref,
                wo_v, x_v, pair_r, comb, sp_r, scr, part, tp_r, gath,
                wo_sem, x_sem, pair_ss, pair_rs, sp_ss, sp_rs, tp_ss, tp_rs, ag_ss, ag_rs, dd_ss, dd_rs):
    y = lax.axis_index('tp')
    s = lax.axis_index('sp')
    xc = s // 2
    c = s % 2
    slab_rows, dim = comb.shape[1], comb.shape[2]
    row_block = (slab_rows - 2 * heads) // heads
    sub = row_block // RING
    width = part.shape[2]
    stat = row_block * heads

    def chip(dx, dy):
        return {'tp': (y + dy) % RING, 'sp': ((xc + dx) % RING) * 2 + c}

    partner = {'sp': xc * 2 + (1 - c)}

    barrier = pltpu.get_barrier_semaphore()
    pl.semaphore_signal(barrier, inc=1, device_id=partner, device_id_type=MESH)
    for k in range(1, RING):
        pl.semaphore_signal(barrier, inc=1, device_id=chip(k, 0), device_id_type=MESH)
        pl.semaphore_signal(barrier, inc=1, device_id=chip(0, k), device_id_type=MESH)

    wo_rows = wo_v.shape[0] // RING
    wo_copies = []
    for i in range(RING):
        rows = pl.ds(i * wo_rows, wo_rows)
        wo_copies.append(pltpu.make_async_copy(wo_hbm.at[rows], wo_v.at[rows], wo_sem.at[i]))
        wo_copies[-1].start()
    x_copy = pltpu.make_async_copy(x_hbm.at[pl.ds(pl.multiple_of(s * row_block, row_block), row_block)], x_v, x_sem)
    x_copy.start()

    pl.semaphore_wait(barrier, 2 * RING - 1)

    order = (2, 1, 3, 0)
    pair = []
    for k in order:
        there = (xc + k) % RING
        pair.append(pltpu.make_async_remote_copy(
            src_ref=o_ref.at[(1 - c) * RING + there], dst_ref=pair_r.at[there],
            send_sem=pair_ss.at[k], recv_sem=pair_rs.at[k], device_id=partner, device_id_type=MESH))
        pair[-1].start()
    sp_copies = {}
    for i, k in enumerate(order):
        there = (xc + k) % RING
        mine = c * RING + there
        pair[i].wait_recv()
        m0 = o_ref[mine, pl.ds(stat, heads), :]
        l0 = o_ref[mine, pl.ds(stat + heads, heads), :]
        m1 = pair_r[there, pl.ds(stat, heads), :]
        l1 = pair_r[there, pl.ds(stat + heads, heads), :]
        top = jnp.maximum(m0, m1)
        f0 = jnp.exp(m0 - top)
        f1 = jnp.exp(m1 - top)
        comb[there, pl.ds(stat, heads), :] = top
        comb[there, pl.ds(stat + heads, heads), :] = l0 * f0 + l1 * f1
        for j in range(row_block):
            rows = pl.ds(j * heads, heads)
            comb[there, rows, :] = o_ref[mine, rows, :] * f0[:, j:j + 1] + pair_r[there, rows, :] * f1[:, j:j + 1]
        if k:
            sp_copies[k] = pltpu.make_async_remote_copy(
                src_ref=comb.at[there], dst_ref=sp_r.at[RING - k - 1],
                send_sem=sp_ss.at[k - 1], recv_sem=sp_rs.at[RING - k - 1], device_id=chip(k, 0), device_id_type=MESH)
            sp_copies[k].start()

    def arrived(k):
        return pltpu.make_async_remote_copy(
            src_ref=comb.at[xc], dst_ref=sp_r.at[k - 1], send_sem=sp_ss.at[k - 1], recv_sem=sp_rs.at[k - 1],
            device_id=chip(k, 0), device_id_type=MESH)
    for k in (1, 3, 2):
        arrived(k).wait_recv()
    m_all = [comb[xc, pl.ds(stat, heads), :]] + [sp_r[k, pl.ds(stat, heads), :] for k in range(RING - 1)]
    l_all = [comb[xc, pl.ds(stat + heads, heads), :]] + [sp_r[k, pl.ds(stat + heads, heads), :] for k in range(RING - 1)]
    top = functools.reduce(jnp.maximum, m_all)
    f_all = [jnp.exp(m - top) for m in m_all]
    total = sum(l * f for l, f in zip(l_all, f_all))
    lane = lax.broadcasted_iota(jnp.int32, total.shape, 1)
    inv = 1.0 / jnp.where(lane < row_block, total, 1.0)
    f_all = [f * inv for f in f_all]
    for j in range(row_block):
        rows = pl.ds(j * heads, heads)
        acc = comb[xc, rows, :] * f_all[0][:, j:j + 1]
        for k in range(RING - 1):
            acc += sp_r[k, rows, :] * f_all[k + 1][:, j:j + 1]
        scr[rows, :] = acc
    attn = jnp.concatenate([scr[pl.ds(h, row_block, stride=heads), :].astype(jnp.bfloat16) for h in range(heads)], axis=1)

    for copy in wo_copies:
        copy.wait()
    n_chunk = tp_ss.shape[0] // (RING - 1)
    cols = width // n_chunk
    tp_copies = []
    for n in range(n_chunk):
        span = pl.ds(n * cols, cols)
        prod = jnp.dot(attn, wo_v[:, span], preferred_element_type=jnp.float32)
        for t in range(RING):
            part[t, :, span] = prod[t * sub:(t + 1) * sub]
        for k in (2, 1, 3):
            to = (y + k) % RING
            copy = pltpu.make_async_remote_copy(
                src_ref=part.at[to, :, span], dst_ref=tp_r.at[RING - k - 1, :, span],
                send_sem=tp_ss.at[n * (RING - 1) + k - 1], recv_sem=tp_rs.at[n * (RING - 1) + RING - k - 1],
                device_id=chip(0, k), device_id_type=MESH)
            copy.start()
            tp_copies.append(copy)
    x_copy.wait()
    for copy in tp_copies:
        copy.wait_recv()
    ssq = jnp.zeros((sub, 1), jnp.float32)
    u_all = []
    for n in range(n_chunk):
        span = pl.ds(n * cols, cols)
        u = part[y, :, span]
        for k in range(RING - 1):
            u += tp_r[k, :, span]
        ssq += jnp.sum(u * u, axis=1, keepdims=True)
        u_all.append(u)
    scale = lax.rsqrt(ssq / width + NORM_EPS)

    a, b = xc * (1 - c) + y * c, y * (1 - c) + xc * c

    def place(da, db):
        return c * RING * RING + ((a + da) % RING) * RING + (b + db) % RING

    for n in range(n_chunk):
        span = pl.ds(n * cols, cols)
        x16 = x_v[:, span].astype(jnp.float32)
        x4 = x16[0:sub]
        for t in range(1, RING):
            x4 = jnp.where(y == t, x16[t * sub:(t + 1) * sub], x4)
        gath[place(0, 0), :, span] = x4 + u_all[n] * scale * (1.0 + wpost_ref[:, span])

    def device(da, db):
        return chip(da * (1 - c) + db * c, db * (1 - c) + da * c)

    half = width // 2
    parts = {'': pl.ds(0, width), 'a': pl.ds(0, half), 'b': pl.ds(half, half)}

    def message(src, part_key, to, number):
        ref = gath.at[place(*src), :, parts[part_key]]
        return pltpu.make_async_remote_copy(
            src_ref=ref, dst_ref=ref, send_sem=ag_ss.at[number], recv_sem=ag_rs.at[number],
            device_id=device(*to), device_id_type=MESH)

    sent = []

    def send(*args):
        copy = message(*args)
        copy.start()
        sent.append(copy)

    def wait(src, part_key, number):
        message(src, part_key, (0, 0), number).wait_recv()

    def to_pair(da, db):
        ref = gath.at[place(da, db)]
        number = da % RING * RING + db % RING
        copy = pltpu.make_async_remote_copy(
            src_ref=ref, dst_ref=ref, send_sem=dd_ss.at[number], recv_sem=dd_rs.at[number],
            device_id=partner, device_id_type=MESH)
        copy.start()
        sent.append(copy)

    unit = {'own': (0, ''), 'prev': (-1, ''), 'next': (1, ''), 'diag_a': (2, 'a'), 'diag_b': (2, 'b')}

    def second(name):
        da, key = unit[name]
        for d in (1, -1):
            send((da, 0), key, (0, d), SECOND[name, d])

    def got_second(name, d):
        da, key = unit[name]
        wait((da, -d), key, SECOND[name, d])

    def forward(da, d, key, name):
        send((da, -d), key, (0, d), FORWARD[name])

    send((0, 0), '', (1, 0), FIRST_P)
    send((0, 0), '', (-1, 0), FIRST_M)
    second('own')
    to_pair(0, 0)
    wait((-1, 0), '', FIRST_P)
    send((-1, 0), 'a', (1, 0), DIAG_A)
    second('prev')
    to_pair(-1, 0)
    wait((1, 0), '', FIRST_M)
    send((1, 0), 'b', (-1, 0), DIAG_B)
    second('next')
    to_pair(1, 0)
    got_second('own', 1)
    forward(0, 1, 'a', 'own_a')
    to_pair(0, -1)
    got_second('own', -1)
    forward(0, -1, 'b', 'own_b')
    to_pair(0, 1)
    wait((2, 0), 'a', DIAG_A)
    second('diag_a')
    wait((2, 0), 'b', DIAG_B)
    second('diag_b')
    to_pair(2, 0)
    got_second('prev', 1)
    forward(-1, 1, '', 'prev')
    to_pair(-1, -1)
    got_second('next', -1)
    forward(1, -1, '', 'next')
    to_pair(1, 1)
    got_second('prev', -1)
    to_pair(-1, 1)
    got_second('next', 1)
    to_pair(1, -1)
    wait((0, 2), 'a', FORWARD['own_a'])
    wait((0, 2), 'b', FORWARD['own_b'])
    to_pair(0, 2)
    got_second('diag_a', 1)
    forward(2, 1, 'a', 'diag_a')
    got_second('diag_b', -1)
    forward(2, -1, 'b', 'diag_b')
    got_second('diag_b', 1)
    to_pair(2, -1)
    got_second('diag_a', -1)
    to_pair(2, 1)
    wait((-1, 2), '', FORWARD['prev'])
    to_pair(-1, 2)
    wait((1, 2), '', FORWARD['next'])
    to_pair(1, 2)
    wait((2, 2), 'a', FORWARD['diag_a'])
    wait((2, 2), 'b', FORWARD['diag_b'])
    to_pair(2, 2)

    a2, b2 = b, a
    for da in range(RING):
        for db in range(RING):
            ref = gath.at[(1 - c) * RING * RING + ((a2 + da) % RING) * RING + (b2 + db) % RING]
            pltpu.make_async_remote_copy(
                src_ref=ref, dst_ref=ref, send_sem=dd_ss.at[da * RING + db], recv_sem=dd_rs.at[da * RING + db],
                device_id=partner, device_id_type=MESH).wait_recv()

    for cx in range(RING):
        for cc in range(2):
            rows = pl.ds((2 * cx + cc) * row_block, row_block)
            for n in range(n_chunk):
                span = pl.ds(n * cols, cols)
                blocks = [gath[cx * RING + t if cc == 0 else RING * RING + t * RING + cx, :, span] for t in range(RING)]
                out_ref[rows, span] = jnp.concatenate(blocks, axis=0).astype(out_ref.dtype)

    for copy in pair:
        copy.wait_send()
    for copy in list(sp_copies.values()) + tp_copies + sent:
        copy.wait_send()


def attend_kernel(kv_heads, pos_ref, x_ref, wpre_ref, cos_ref, sin_ref, wq_hbm, wk_hbm, wv_hbm, kc_hbm, vc_hbm,
                  pack_ref, ko_hbm, vo_hbm, a_v, w_v, q_s, kn_s, vn_s, ko_ref, vo_ref, w_sem, k_sem, v_sem, ko_sem, vo_sem):
    rows, width = x_ref.shape
    dim = pack_ref.shape[2]
    n_slab = pack_ref.shape[0]
    row_block = rows // n_slab
    heads = q_s.shape[0] // rows
    group = heads // kv_heads
    span = ko_ref.shape[1]
    seq_block = span // kv_heads
    window = kn_s.shape[0] // rows
    chunk = w_v.shape[2]
    first_pos = lax.axis_index('sp') * seq_block

    jobs = [('k', wk_hbm, i) for i in range(wk_hbm.shape[1] // chunk)]
    jobs += [('v', wv_hbm, i) for i in range(wv_hbm.shape[1] // chunk)]
    jobs += [('q', wq_hbm, i) for i in range(wq_hbm.shape[1] // chunk)]

    def w_copy(n):
        _, ref, i = jobs[n]
        return pltpu.make_async_copy(ref.at[:, pl.ds(i * chunk, chunk)], w_v.at[n], w_sem.at[n])

    def slab_copies(d):
        part = pl.ds(d * row_block, row_block)
        return (pltpu.make_async_copy(kc_hbm.at[part], ko_ref.at[part], k_sem.at[d]),
                pltpu.make_async_copy(vc_hbm.at[part], vo_ref.at[part], v_sem.at[d]))

    def out_copies(d):
        part = pl.ds(d * row_block, row_block)
        return (pltpu.make_async_copy(ko_ref.at[part], ko_hbm.at[part], ko_sem.at[d]),
                pltpu.make_async_copy(vo_ref.at[part], vo_hbm.at[part], vo_sem.at[d]))

    for n in range(len(jobs)):
        w_copy(n).start()

    n_piece = 6 if width % (6 * 128) == 0 else 1
    piece = width // n_piece

    @pl.loop(0, rows // 16)
    def _(i):
        part = pl.ds(pl.multiple_of(i * 16, 16), 16)
        ssq = jnp.zeros((16, 1), jnp.float32)
        for n in range(n_piece):
            xf = x_ref[part, pl.ds(n * piece, piece)].astype(jnp.float32)
            ssq += jnp.sum(xf * xf, axis=1, keepdims=True)
        scale = lax.rsqrt(ssq / width + NORM_EPS)
        for n in range(n_piece):
            cols = pl.ds(n * piece, piece)
            xf = x_ref[part, cols].astype(jnp.float32)
            a_v[part, cols] = (xf * scale * (1.0 + wpre_ref[:, cols])).astype(a_v.dtype)

    half = dim // 2
    cos_all = jnp.concatenate([cos_ref[...], cos_ref[...]], axis=1)
    sin_all = jnp.concatenate([-sin_ref[...], sin_ref[...]], axis=1)
    slabs_started = 0
    for n, (kind, _, i) in enumerate(jobs):
        w_copy(n).wait()
        upto = n_slab * (n + 1) // len(jobs)
        for d in range(slabs_started, upto):
            for copy in slab_copies(d):
                copy.start()
        slabs_started = upto
        prod = jnp.dot(a_v[...], w_v[n], preferred_element_type=jnp.float32)
        for h in range(chunk // dim):
            val = prod[:, h * dim:(h + 1) * dim]
            if kind != 'v':
                val = val * cos_all + pltpu.roll(val, half, 1) * sin_all
            head = i * (chunk // dim) + h
            if kind == 'q':
                q_s[pl.ds(head, rows, stride=heads), :] = val
            else:
                for r in range(window // kv_heads):
                    (kn_s if kind == 'k' else vn_s)[pl.ds(r * kv_heads + head, rows, stride=window), :] = val

    col = lax.broadcasted_iota(jnp.int32, (heads, span), 1)
    row = lax.broadcasted_iota(jnp.int32, (heads, span), 0)
    same_head = col % kv_heads == row // group
    lane = lax.broadcasted_iota(jnp.int32, (heads, dim), 1)
    win_time = lax.broadcasted_iota(jnp.int32, (window, dim), 0) // kv_heads
    per_window = window // kv_heads

    @pl.loop(0, n_slab)
    def _(d):
        for copy in slab_copies(d):
            copy.wait()
        last = []
        for j in range(row_block):
            b = d * row_block + j
            here = pos_ref[b] - first_pos
            last.append(here)
            slot = jnp.clip(here, 0, seq_block - 1)
            at = pl.ds(pl.multiple_of(slot // per_window * window, window), window)
            hit = win_time == jnp.where(here == slot, slot % per_window, -1)
            new = pl.ds(pl.multiple_of(b * window, window), window)
            ko_ref[b, at, :] = jnp.where(hit, kn_s[new, :], ko_ref[b, at, :].astype(jnp.float32)).astype(ko_ref.dtype)
            vo_ref[b, at, :] = jnp.where(hit, vn_s[new, :], vo_ref[b, at, :].astype(jnp.float32)).astype(vo_ref.dtype)
        for copy in out_copies(d):
            copy.start()
        scores = []
        for j in range(row_block):
            b = d * row_block + j
            q_b = q_s[pl.ds(pl.multiple_of(b * heads, heads), heads), :].astype(jnp.bfloat16)
            scores.append(lax.dot_general(q_b, ko_ref[b], (((1,), (1,)), ((), ())), preferred_element_type=jnp.float32))
        tops = jnp.zeros((heads, dim), jnp.float32)
        sums = jnp.zeros((heads, dim), jnp.float32)
        weights = []
        for j in range(row_block):
            valid = same_head & (col < (last[j] + 1) * kv_heads)
            capped = jnp.where(valid, SOFT_CAP * jnp.tanh(scores[j] * (dim ** -0.5 / SOFT_CAP)), NEG_FILL)
            top = jnp.max(capped, axis=1, keepdims=True)
            exp_w = jnp.where(valid, jnp.exp(capped - top), 0.0)
            tops = jnp.where(lane == j, top, tops)
            sums = jnp.where(lane == j, jnp.sum(exp_w, axis=1, keepdims=True), sums)
            weights.append(exp_w.astype(jnp.bfloat16))
        slab = d % 2 * (n_slab // 2) + d // 2
        for j in range(row_block):
            b = d * row_block + j
            pack_ref[slab, pl.ds(j * heads, heads), :] = jnp.dot(weights[j], vo_ref[b], preferred_element_type=jnp.float32)
        pack_ref[slab, pl.ds(row_block * heads, heads), :] = tops
        pack_ref[slab, pl.ds((row_block + 1) * heads, heads), :] = sums

    for d in range(n_slab):
        for copy in out_copies(d):
            copy.wait()


def gain_row(gain_w):
    return jnp.pad(gain_w, (0, -gain_w.shape[0] % 1024 + 1024))[None]


def attend(x_in, cur_pos, w_pre, w_q, w_k, w_v, k_cache, v_cache, n_sp):
    rows, seq_block, kv_heads, dim = k_cache.shape
    width = x_in.shape[1]
    heads = w_q.shape[1] // dim
    chunk = 2 * dim
    window = 16
    n_jobs = (w_q.shape[1] + w_k.shape[1] + w_v.shape[1]) // chunk
    inv_freq = ROPE_BASE ** (-2.0 * jnp.arange(dim // 2, dtype=jnp.float32) / dim)
    angles = cur_pos.astype(jnp.float32)[:, None] * inv_freq[None, :]
    flat = (rows, seq_block * kv_heads, dim)
    sems = pltpu.SemaphoreType.DMA
    vmem = pl.BlockSpec(memory_space=pltpu.VMEM)
    hbm = pl.BlockSpec(memory_space=pltpu.HBM)
    pack, k_out, v_out = pl.pallas_call(
        functools.partial(attend_kernel, kv_heads),
        out_shape=(jax.ShapeDtypeStruct((n_sp, rows // n_sp * heads + 2 * heads, dim), jnp.float32),
                   jax.ShapeDtypeStruct(flat, k_cache.dtype), jax.ShapeDtypeStruct(flat, v_cache.dtype)),
        in_specs=[pl.BlockSpec(memory_space=pltpu.SMEM), vmem, vmem, vmem, vmem, hbm, hbm, hbm, hbm, hbm],
        out_specs=(vmem, hbm, hbm),
        scratch_shapes=[
            pltpu.VMEM((rows, width), jnp.bfloat16),
            pltpu.VMEM((n_jobs, width, chunk), w_q.dtype),
            pltpu.VMEM(((rows + 1) * heads, dim), jnp.float32),
            pltpu.VMEM(((rows + 1) * window, dim), jnp.float32),
            pltpu.VMEM(((rows + 1) * window, dim), jnp.float32),
            pltpu.VMEM(flat, k_cache.dtype),
            pltpu.VMEM(flat, v_cache.dtype),
            sems((n_jobs,)), sems((n_sp,)), sems((n_sp,)), sems((n_sp,)), sems((n_sp,)),
        ],
        compiler_params=pltpu.CompilerParams(vmem_limit_bytes=48 * 2**20),
        cost_estimate=pl.CostEstimate(flops=2 * rows * w_q.size * 2, bytes_accessed=w_q.size * 4 + k_cache.size * 4, transcendentals=0),
        name='attend',
    )(cur_pos, x_in, gain_row(w_pre), jnp.cos(angles), jnp.sin(angles), w_q, w_k, w_v, k_cache.reshape(flat), v_cache.reshape(flat))
    return pack, k_out.reshape(k_cache.shape), v_out.reshape(v_cache.shape)


def finish(o_pack, w_o, x_in, w_post, heads):
    rows, width = x_in.shape
    _, slab_rows, dim = o_pack.shape
    row_block = rows // (2 * RING)
    n_chunk = 3 if width % (3 * 256) == 0 else 1
    sems = pltpu.SemaphoreType.DMA
    vmem = pl.BlockSpec(memory_space=pltpu.VMEM)
    return pl.pallas_call(
        functools.partial(comm_kernel, heads),
        out_shape=jax.ShapeDtypeStruct((rows, width), x_in.dtype),
        in_specs=[vmem, pl.BlockSpec(memory_space=pltpu.HBM), pl.BlockSpec(memory_space=pltpu.HBM), vmem],
        out_specs=vmem,
        scratch_shapes=[
            pltpu.VMEM(w_o.shape, w_o.dtype),
            pltpu.VMEM((row_block, width), x_in.dtype),
            pltpu.VMEM((RING, slab_rows, dim), jnp.float32),
            pltpu.VMEM((RING, slab_rows, dim), jnp.float32),
            pltpu.VMEM((RING - 1, slab_rows, dim), jnp.float32),
            pltpu.VMEM(((row_block + 1) * heads, dim), jnp.float32),
            pltpu.VMEM((RING, row_block // RING, width), jnp.float32),
            pltpu.VMEM((RING - 1, row_block // RING, width), jnp.float32),
            pltpu.VMEM((2 * RING * RING, row_block // RING, width), jnp.float32),
            sems((RING,)), sems(()),
            sems((RING,)), sems((RING,)),
            sems((RING - 1,)), sems((RING - 1,)),
            sems((n_chunk * (RING - 1),)), sems((n_chunk * (RING - 1),)),
            sems((N_GATHER,)), sems((N_GATHER,)),
            sems((RING * RING,)), sems((RING * RING,)),
        ],
        compiler_params=pltpu.CompilerParams(collective_id=0, has_side_effects=True, vmem_limit_bytes=22 * 2**20),
        cost_estimate=pl.CostEstimate(flops=2 * rows * w_o.size // 8, bytes_accessed=w_o.size * 2, transcendentals=0),
        name='finish',
    )(o_pack, pltpu.with_memory_space_constraint(w_o, pltpu.HBM), x_in, gain_row(w_post))


def solution(mesh):
    cache_spec = P('dp', 'sp', 'tp', None)
    n_sp = mesh.shape['sp']
    assert n_sp == 2 * RING and mesh.shape['tp'] == RING

    def local_step(x_in, cur_pos, w_pre, w_q, w_k, w_v, w_o, w_post, k_cache, v_cache):
        heads_local = w_q.shape[1] // k_cache.shape[3]
        slabs, k_out, v_out = attend(x_in, cur_pos, w_pre, w_q, w_k, w_v, k_cache, v_cache, n_sp)
        x_out = finish(slabs, w_o, x_in, w_post, heads_local)
        return x_out, k_out, v_out

    return jax.shard_map(local_step, mesh=mesh,
                         in_specs=(P('dp', None), P('dp'), P(None), P(None, 'tp'), P(None, 'tp'), P(None, 'tp'), P('tp', None), P(None), cache_spec, cache_spec),
                         out_specs=(P('dp', None), cache_spec, cache_spec), check_vma=False)
```

```python
import functools

import jax
import jax.numpy as jnp
from jax import lax
from jax.experimental import pallas as pl
from jax.experimental.pallas import tpu as pltpu
from jax.sharding import PartitionSpec as P

SOFT_CAP = 50.0
ROPE_BASE = 10000.0
NORM_EPS = 1e-6
NEG_FILL = -1e30
MESH = pl.DeviceIdType.MESH
RING = 4


N_GATHER = 30


def comm_kernel(heads, o_ref, wo_hbm, x_hbm, wpost_hbm, out_ref,
                wo_v, x_v, wpost_ref, pair_r, comb, sp_r, scr, part, tp_r, gath,
                wo_sem, x_sem, pair_ss, pair_rs, sp_ss, sp_rs, tp_ss, tp_rs, ag_ss, ag_rs, dd_ss, dd_rs):
    y = lax.axis_index('tp')
    s = lax.axis_index('sp')
    xc = s // 2
    c = s % 2
    slab_rows, dim = comb.shape[1], comb.shape[2]
    row_block = (slab_rows - 2 * heads) // heads
    sub = row_block // RING
    width = part.shape[2]
    stat = row_block * heads

    def chip(dx, dy):
        return {'tp': (y + dy) % RING, 'sp': ((xc + dx) % RING) * 2 + c}

    partner = {'sp': xc * 2 + (1 - c)}

    barrier = pltpu.get_barrier_semaphore()
    pl.semaphore_signal(barrier, inc=1, device_id=partner, device_id_type=MESH)
    for k in range(1, RING):
        pl.semaphore_signal(barrier, inc=1, device_id=chip(k, 0), device_id_type=MESH)
        pl.semaphore_signal(barrier, inc=1, device_id=chip(0, k), device_id_type=MESH)

    wo_rows = wo_v.shape[0] // RING
    wo_copies = []
    for i in range(RING):
        rows = pl.ds(i * wo_rows, wo_rows)
        wo_copies.append(pltpu.make_async_copy(wo_hbm.at[rows], wo_v.at[rows], wo_sem.at[i]))
        wo_copies[-1].start()
    x_copy = pltpu.make_async_copy(x_hbm.at[pl.ds(pl.multiple_of(s * row_block, row_block), row_block)], x_v, x_sem.at[0])
    x_copy.start()
    gain_copy = pltpu.make_async_copy(wpost_hbm, wpost_ref, x_sem.at[1])
    gain_copy.start()

    pl.semaphore_wait(barrier, 2 * RING - 1)

    order = (2, 1, 3, 0)
    pair = []
    for k in order:
        there = (xc + k) % RING
        pair.append(pltpu.make_async_remote_copy(
            src_ref=o_ref.at[(1 - c) * RING + there], dst_ref=pair_r.at[there],
            send_sem=pair_ss.at[k], recv_sem=pair_rs.at[k], device_id=partner, device_id_type=MESH))
        pair[-1].start()
    sp_copies = {}
    for i, k in enumerate(order):
        there = (xc + k) % RING
        mine = c * RING + there
        pair[i].wait_recv()
        m0 = o_ref[mine, pl.ds(stat, heads), :]
        l0 = o_ref[mine, pl.ds(stat + heads, heads), :]
        m1 = pair_r[there, pl.ds(stat, heads), :]
        l1 = pair_r[there, pl.ds(stat + heads, heads), :]
        top = jnp.maximum(m0, m1)
        f0 = jnp.exp(m0 - top)
        f1 = jnp.exp(m1 - top)
        comb[there, pl.ds(stat, heads), :] = top
        comb[there, pl.ds(stat + heads, heads), :] = l0 * f0 + l1 * f1
        for j in range(row_block):
            rows = pl.ds(j * heads, heads)
            comb[there, rows, :] = o_ref[mine, rows, :] * f0[:, j:j + 1] + pair_r[there, rows, :] * f1[:, j:j + 1]
        if k:
            sp_copies[k] = pltpu.make_async_remote_copy(
                src_ref=comb.at[there], dst_ref=sp_r.at[RING - k - 1],
                send_sem=sp_ss.at[k - 1], recv_sem=sp_rs.at[RING - k - 1], device_id=chip(k, 0), device_id_type=MESH)
            sp_copies[k].start()

    def arrived(k):
        return pltpu.make_async_remote_copy(
            src_ref=comb.at[xc], dst_ref=sp_r.at[k - 1], send_sem=sp_ss.at[k - 1], recv_sem=sp_rs.at[k - 1],
            device_id=chip(k, 0), device_id_type=MESH)
    for k in (1, 3, 2):
        arrived(k).wait_recv()
    m_all = [comb[xc, pl.ds(stat, heads), :]] + [sp_r[k, pl.ds(stat, heads), :] for k in range(RING - 1)]
    l_all = [comb[xc, pl.ds(stat + heads, heads), :]] + [sp_r[k, pl.ds(stat + heads, heads), :] for k in range(RING - 1)]
    top = functools.reduce(jnp.maximum, m_all)
    f_all = [jnp.exp(m - top) for m in m_all]
    total = sum(l * f for l, f in zip(l_all, f_all))
    lane = lax.broadcasted_iota(jnp.int32, total.shape, 1)
    inv = 1.0 / jnp.where(lane < row_block, total, 1.0)
    f_all = [f * inv for f in f_all]
    for j in range(row_block):
        rows = pl.ds(j * heads, heads)
        acc = comb[xc, rows, :] * f_all[0][:, j:j + 1]
        for k in range(RING - 1):
            acc += sp_r[k, rows, :] * f_all[k + 1][:, j:j + 1]
        scr[rows, :] = acc
    attn = jnp.concatenate([scr[pl.ds(h, row_block, stride=heads), :].astype(jnp.bfloat16) for h in range(heads)], axis=1)

    for copy in wo_copies:
        copy.wait()
    n_chunk = tp_ss.shape[0] // (RING - 1)
    cols = width // n_chunk
    tp_copies = []
    for n in range(n_chunk):
        span = pl.ds(n * cols, cols)
        prod = jnp.dot(attn, wo_v[:, span], preferred_element_type=jnp.float32)
        for t in range(RING):
            part[t, :, span] = prod[t * sub:(t + 1) * sub]
        for k in (2, 1, 3):
            to = (y + k) % RING
            copy = pltpu.make_async_remote_copy(
                src_ref=part.at[to, :, span], dst_ref=tp_r.at[RING - k - 1, :, span],
                send_sem=tp_ss.at[n * (RING - 1) + k - 1], recv_sem=tp_rs.at[n * (RING - 1) + RING - k - 1],
                device_id=chip(0, k), device_id_type=MESH)
            copy.start()
            tp_copies.append(copy)
    x_copy.wait()
    gain_copy.wait()
    for copy in tp_copies:
        copy.wait_recv()
    ssq = jnp.zeros((sub, 1), jnp.float32)
    u_all = []
    for n in range(n_chunk):
        span = pl.ds(n * cols, cols)
        u = part[y, :, span]
        for k in range(RING - 1):
            u += tp_r[k, :, span]
        ssq += jnp.sum(u * u, axis=1, keepdims=True)
        u_all.append(u)
    scale = lax.rsqrt(ssq / width + NORM_EPS)

    a, b = xc * (1 - c) + y * c, y * (1 - c) + xc * c

    def place(da, db):
        return c * RING * RING + ((a + da) % RING) * RING + (b + db) % RING

    per = cols // dim
    for n in range(n_chunk):
        for i in range(per):
            span = pl.ds(n * cols + i * dim, dim)
            x16 = x_v[:, span].astype(jnp.float32)
            x4 = x16[0:sub]
            for t in range(1, RING):
                x4 = jnp.where(y == t, x16[t * sub:(t + 1) * sub], x4)
            gain = 1.0 + wpost_ref[n * per + i:n * per + i + 1, :]
            gath[place(0, 0), :, span] = x4 + u_all[n][:, i * dim:(i + 1) * dim] * scale * gain

    def device(da, db):
        return chip(da * (1 - c) + db * c, db * (1 - c) + da * c)

    half = width // 2
    sent = []

    def message(src, h, to, number):
        ref = gath.at[place(*src), :, pl.ds(h * half, half)]
        return pltpu.make_async_remote_copy(
            src_ref=ref, dst_ref=ref, send_sem=ag_ss.at[number], recv_sem=ag_rs.at[number],
            device_id=device(*to), device_id_type=MESH)

    def send(*args):
        copy = message(*args)
        copy.start()
        sent.append(copy)

    def wait(src, h, number):
        message(src, h, (0, 0), number).wait_recv()

    def to_pair(da, db):
        ref = gath.at[place(da, db)]
        number = da % RING * RING + db % RING
        copy = pltpu.make_async_remote_copy(
            src_ref=ref, dst_ref=ref, send_sem=dd_ss.at[number], recv_sem=dd_rs.at[number],
            device_id=partner, device_id_type=MESH)
        copy.start()
        sent.append(copy)

    sign = (1, -1)

    def first(h, d):
        send((0, 0), h, (d, 0), first_no[h, d])

    def second(da, h):
        for d in sign:
            send((da, 0), h, (0, d), second_no[da % RING, h, d])

    def got_second(da, h):
        for d in (sign[h], -sign[h]):
            wait((da, -d), h, second_no[da % RING, h, d])
            if d == sign[h]:
                send((da, -d), h, (0, d), forward_no[da % RING, h])

    def pairs(da):
        to_pair(da, -1)
        to_pair(da, 1)

    numbers = iter(range(N_GATHER))
    first_no = {(h, d): next(numbers) for h in (0, 1) for d in sign}
    diag_no = {h: next(numbers) for h in (0, 1)}
    second_no = {(k, h, d): next(numbers) for k in range(RING) for h in (0, 1) for d in sign}
    forward_no = {(k, h): next(numbers) for k in range(RING) for h in (0, 1)}

    for h in (0, 1):
        first(h, 1)
        first(h, -1)
        second(0, h)
    to_pair(0, 0)
    for h in (0, 1):
        for d in (sign[h], -sign[h]):
            wait((-d, 0), h, first_no[h, d])
            if d == sign[h]:
                send((-d, 0), h, (d, 0), diag_no[h])
            second(-d, h)
    to_pair(-1, 0)
    to_pair(1, 0)
    for h in (0, 1):
        got_second(0, h)
    pairs(0)
    for h in (0, 1):
        wait((2, 0), h, diag_no[h])
        second(2, h)
    to_pair(2, 0)
    for h in (0, 1):
        got_second(-1, h)
        got_second(1, h)
    pairs(-1)
    pairs(1)
    for h in (0, 1):
        wait((0, 2), h, forward_no[0, h])
    to_pair(0, 2)
    for h in (0, 1):
        got_second(2, h)
    pairs(2)
    for k in (-1, 1, 2):
        for h in (0, 1):
            wait((k, 2), h, forward_no[k % RING, h])
        to_pair(k, 2)

    def from_pair(da, db):
        ref = gath.at[(1 - c) * RING * RING + ((b + da) % RING) * RING + (a + db) % RING]
        number = da % RING * RING + db % RING
        pltpu.make_async_remote_copy(
            src_ref=ref, dst_ref=ref, send_sem=dd_ss.at[number], recv_sem=dd_rs.at[number],
            device_id=partner, device_id_type=MESH).wait_recv()

    for da in range(RING):
        for db in range(RING):
            from_pair(da, db)

    for cx in range(RING):
        for cc in range(2):
            rows = pl.ds((2 * cx + cc) * row_block, row_block)
            for n in range(n_chunk):
                span = pl.ds(n * cols, cols)
                blocks = [gath[cx * RING + t if cc == 0 else RING * RING + t * RING + cx, :, span] for t in range(RING)]
                out_ref[rows, span] = jnp.concatenate(blocks, axis=0).astype(out_ref.dtype)

    for copy in pair:
        copy.wait_send()
    for copy in list(sp_copies.values()) + tp_copies + sent:
        copy.wait_send()


def attend_kernel(kv_heads, freq_ref, pos_hbm, x_hbm, wpre_hbm, wq_hbm, wk_hbm, wv_hbm, kc_hbm, vc_hbm,
                  pack_ref, ko_hbm, vo_hbm, pos_ref, posv_ref, x_ref, wpre_ref, a_v, w_v, q_s, kn_s, vn_s, ko_ref, vo_ref, in_sem, w_sem, k_sem, v_sem, ko_sem, vo_sem):
    rows, width = x_ref.shape
    dim = pack_ref.shape[2]
    n_slab = pack_ref.shape[0]
    row_block = rows // n_slab
    heads = q_s.shape[0] // rows
    group = heads // kv_heads
    span = ko_ref.shape[1]
    seq_block = span // kv_heads
    window = kn_s.shape[0] // rows
    chunk = w_v.shape[2]
    first_pos = lax.axis_index('sp') * seq_block

    jobs = [('k', wk_hbm, i) for i in range(wk_hbm.shape[1] // chunk)]
    jobs += [('v', wv_hbm, i) for i in range(wv_hbm.shape[1] // chunk)]
    jobs += [('q', wq_hbm, i) for i in range(wq_hbm.shape[1] // chunk)]

    def w_copy(n):
        _, ref, i = jobs[n]
        return pltpu.make_async_copy(ref.at[:, pl.ds(i * chunk, chunk)], w_v.at[n], w_sem.at[n])

    def slab_copies(d):
        part = pl.ds(d * row_block, row_block)
        return (pltpu.make_async_copy(kc_hbm.at[part], ko_ref.at[part], k_sem.at[d]),
                pltpu.make_async_copy(vc_hbm.at[part], vo_ref.at[part], v_sem.at[d]))

    def out_copies(d):
        part = pl.ds(d * row_block, row_block)
        return (pltpu.make_async_copy(ko_ref.at[part], ko_hbm.at[part], ko_sem.at[d]),
                pltpu.make_async_copy(vo_ref.at[part], vo_hbm.at[part], vo_sem.at[d]))

    small = [pltpu.make_async_copy(a, b, in_sem.at[i]) for i, (a, b) in enumerate(
        ((x_hbm, x_ref), (wpre_hbm, wpre_ref), (pos_hbm, pos_ref), (pos_hbm, posv_ref)))]
    for copy in small:
        copy.start()
    for n in range(len(jobs)):
        w_copy(n).start()
    for copy in small:
        copy.wait()

    @pl.loop(0, rows // 16)
    def _(i):
        part = pl.ds(pl.multiple_of(i * 16, 16), 16)
        squares = jnp.zeros((16, dim), jnp.float32)
        for n in range(width // dim):
            xf = x_ref[part, pl.ds(n * dim, dim)].astype(jnp.float32)
            squares += xf * xf
        scale = lax.rsqrt(jnp.sum(squares, axis=1, keepdims=True) / width + NORM_EPS)
        for n in range(width // dim):
            cols = pl.ds(n * dim, dim)
            xf = x_ref[part, cols].astype(jnp.float32)
            a_v[part, cols] = (xf * scale * (1.0 + wpre_ref[n:n + 1, :])).astype(a_v.dtype)

    half = dim // 2
    positions = jnp.broadcast_to(posv_ref[...].astype(jnp.float32), (dim, rows)).T
    angles = positions * freq_ref[0:1, :]
    cos_all = jnp.cos(angles)
    sin_all = jnp.sin(angles)
    sin_all = jnp.where(lax.broadcasted_iota(jnp.int32, sin_all.shape, 1) < half, -sin_all, sin_all)
    slabs_started = 0
    for n, (kind, _, i) in enumerate(jobs):
        w_copy(n).wait()
        upto = n_slab * (n + 1) // len(jobs)
        for d in range(slabs_started, upto):
            for copy in slab_copies(d):
                copy.start()
        slabs_started = upto
        prod = jnp.dot(a_v[...], w_v[n], preferred_element_type=jnp.float32)
        for h in range(chunk // dim):
            val = prod[:, h * dim:(h + 1) * dim]
            if kind != 'v':
                val = val * cos_all + pltpu.roll(val, half, 1) * sin_all
            head = i * (chunk // dim) + h
            if kind == 'q':
                q_s[pl.ds(head, rows, stride=heads), :] = val
            else:
                for r in range(window // kv_heads):
                    (kn_s if kind == 'k' else vn_s)[pl.ds(r * kv_heads + head, rows, stride=window), :] = val

    col = lax.broadcasted_iota(jnp.int32, (heads, span), 1)
    row = lax.broadcasted_iota(jnp.int32, (heads, span), 0)
    same_head = col % kv_heads == row // group
    lane = lax.broadcasted_iota(jnp.int32, (heads, dim), 1)
    win_time = lax.broadcasted_iota(jnp.int32, (window, dim), 0) // kv_heads
    per_window = window // kv_heads

    @pl.loop(0, n_slab)
    def _(d):
        for copy in slab_copies(d):
            copy.wait()
        last = []
        for j in range(row_block):
            b = d * row_block + j
            here = pos_ref[0, b] - first_pos
            last.append(here)
            slot = jnp.clip(here, 0, seq_block - 1)
            at = pl.ds(pl.multiple_of(slot // per_window * window, window), window)
            hit = win_time == jnp.where(here == slot, slot % per_window, -1)
            new = pl.ds(pl.multiple_of(b * window, window), window)
            ko_ref[b, at, :] = jnp.where(hit, kn_s[new, :], ko_ref[b, at, :].astype(jnp.float32)).astype(ko_ref.dtype)
            vo_ref[b, at, :] = jnp.where(hit, vn_s[new, :], vo_ref[b, at, :].astype(jnp.float32)).astype(vo_ref.dtype)
        for copy in out_copies(d):
            copy.start()
        scores = []
        for j in range(row_block):
            b = d * row_block + j
            q_b = q_s[pl.ds(pl.multiple_of(b * heads, heads), heads), :].astype(jnp.bfloat16)
            scores.append(lax.dot_general(q_b, ko_ref[b], (((1,), (1,)), ((), ())), preferred_element_type=jnp.float32))
        tops = jnp.zeros((heads, dim), jnp.float32)
        sums = jnp.zeros((heads, dim), jnp.float32)
        weights = []
        for j in range(row_block):
            valid = same_head & (col < (last[j] + 1) * kv_heads)
            capped = jnp.where(valid, SOFT_CAP * jnp.tanh(scores[j] * (dim ** -0.5 / SOFT_CAP)), NEG_FILL)
            top = jnp.max(capped, axis=1, keepdims=True)
            exp_w = jnp.where(valid, jnp.exp(capped - top), 0.0)
            tops = jnp.where(lane == j, top, tops)
            sums = jnp.where(lane == j, jnp.sum(exp_w, axis=1, keepdims=True), sums)
            weights.append(exp_w.astype(jnp.bfloat16))
        slab = d % 2 * (n_slab // 2) + d // 2
        for j in range(row_block):
            b = d * row_block + j
            pack_ref[slab, pl.ds(j * heads, heads), :] = jnp.dot(weights[j], vo_ref[b], preferred_element_type=jnp.float32)
        pack_ref[slab, pl.ds(row_block * heads, heads), :] = tops
        pack_ref[slab, pl.ds((row_block + 1) * heads, heads), :] = sums

    for d in range(n_slab):
        for copy in out_copies(d):
            copy.wait()


def in_hbm(operand):
    return pltpu.with_memory_space_constraint(operand, pltpu.HBM)


def attend(x_in, cur_pos, w_pre, w_q, w_k, w_v, k_cache, v_cache, n_sp):
    rows, seq_block, kv_heads, dim = k_cache.shape
    width = x_in.shape[1]
    heads = w_q.shape[1] // dim
    chunk = 2 * dim
    window = 16
    n_jobs = (w_q.shape[1] + w_k.shape[1] + w_v.shape[1]) // chunk
    inv_freq = ROPE_BASE ** (-2.0 * jnp.arange(dim // 2, dtype=jnp.float32) / dim)
    freq = jnp.broadcast_to(jnp.concatenate([inv_freq, inv_freq])[None], (8, dim))
    flat = (rows, seq_block * kv_heads, dim)
    sems = pltpu.SemaphoreType.DMA
    vmem = pl.BlockSpec(memory_space=pltpu.VMEM)
    hbm = pl.BlockSpec(memory_space=pltpu.HBM)
    pack, k_out, v_out = pl.pallas_call(
        functools.partial(attend_kernel, kv_heads),
        out_shape=(jax.ShapeDtypeStruct((n_sp, rows // n_sp * heads + 2 * heads, dim), jnp.float32),
                   jax.ShapeDtypeStruct(flat, k_cache.dtype), jax.ShapeDtypeStruct(flat, v_cache.dtype)),
        in_specs=[vmem] + [hbm] * 8,
        out_specs=(vmem, hbm, hbm),
        scratch_shapes=[
            pltpu.SMEM((1, rows), cur_pos.dtype),
            pltpu.VMEM((1, rows), cur_pos.dtype),
            pltpu.VMEM((rows, width), x_in.dtype),
            pltpu.VMEM((width // dim, dim), jnp.float32),
            pltpu.VMEM((rows, width), jnp.bfloat16),
            pltpu.VMEM((n_jobs, width, chunk), w_q.dtype),
            pltpu.VMEM(((rows + 1) * heads, dim), jnp.float32),
            pltpu.VMEM(((rows + 1) * window, dim), jnp.float32),
            pltpu.VMEM(((rows + 1) * window, dim), jnp.float32),
            pltpu.VMEM(flat, k_cache.dtype),
            pltpu.VMEM(flat, v_cache.dtype),
            sems((4,)), sems((n_jobs,)), sems((n_sp,)), sems((n_sp,)), sems((n_sp,)), sems((n_sp,)),
        ],
        compiler_params=pltpu.CompilerParams(vmem_limit_bytes=48 * 2**20),
        cost_estimate=pl.CostEstimate(flops=2 * rows * w_q.size * 2, bytes_accessed=w_q.size * 4 + k_cache.size * 4, transcendentals=0),
        name='attend',
    )(freq, in_hbm(cur_pos[None]), in_hbm(x_in), in_hbm(w_pre.reshape(-1, dim)),
      in_hbm(w_q), in_hbm(w_k), in_hbm(w_v), in_hbm(k_cache.reshape(flat)), in_hbm(v_cache.reshape(flat)))
    return pack, k_out.reshape(k_cache.shape), v_out.reshape(v_cache.shape)


def finish(o_pack, w_o, x_in, w_post, heads):
    rows, width = x_in.shape
    _, slab_rows, dim = o_pack.shape
    row_block = rows // (2 * RING)
    n_chunk = 3 if width % (3 * 256) == 0 else 1
    sems = pltpu.SemaphoreType.DMA
    vmem = pl.BlockSpec(memory_space=pltpu.VMEM)
    hbm = pl.BlockSpec(memory_space=pltpu.HBM)
    return pl.pallas_call(
        functools.partial(comm_kernel, heads),
        out_shape=jax.ShapeDtypeStruct((rows, width), x_in.dtype),
        in_specs=[vmem, hbm, hbm, hbm],
        out_specs=vmem,
        scratch_shapes=[
            pltpu.VMEM(w_o.shape, w_o.dtype),
            pltpu.VMEM((row_block, width), x_in.dtype),
            pltpu.VMEM((width // dim, dim), jnp.float32),
            pltpu.VMEM((RING, slab_rows, dim), jnp.float32),
            pltpu.VMEM((RING, slab_rows, dim), jnp.float32),
            pltpu.VMEM((RING - 1, slab_rows, dim), jnp.float32),
            pltpu.VMEM(((row_block + 1) * heads, dim), jnp.float32),
            pltpu.VMEM((RING, row_block // RING, width), jnp.float32),
            pltpu.VMEM((RING - 1, row_block // RING, width), jnp.float32),
            pltpu.VMEM((2 * RING * RING, row_block // RING, width), jnp.float32),
            sems((RING,)), sems((2,)),
            sems((RING,)), sems((RING,)),
            sems((RING - 1,)), sems((RING - 1,)),
            sems((n_chunk * (RING - 1),)), sems((n_chunk * (RING - 1),)),
            sems((N_GATHER,)), sems((N_GATHER,)),
            sems((RING * RING,)), sems((RING * RING,)),
        ],
        compiler_params=pltpu.CompilerParams(collective_id=0, has_side_effects=True, vmem_limit_bytes=22 * 2**20),
        cost_estimate=pl.CostEstimate(flops=2 * rows * w_o.size // 8, bytes_accessed=w_o.size * 2, transcendentals=0),
        name='finish',
    )(o_pack, in_hbm(w_o), in_hbm(x_in), in_hbm(w_post.reshape(-1, dim)))


def solution(mesh):
    cache_spec = P('dp', 'sp', 'tp', None)
    n_sp = mesh.shape['sp']
    assert n_sp == 2 * RING and mesh.shape['tp'] == RING

    def local_step(x_in, cur_pos, w_pre, w_q, w_k, w_v, w_o, w_post, k_cache, v_cache):
        heads_local = w_q.shape[1] // k_cache.shape[3]
        slabs, k_out, v_out = attend(x_in, cur_pos, w_pre, w_q, w_k, w_v, k_cache, v_cache, n_sp)
        x_out = finish(slabs, w_o, x_in, w_post, heads_local)
        return x_out, k_out, v_out

    return jax.shard_map(local_step, mesh=mesh,
                         in_specs=(P('dp', None), P('dp'), P(None), P(None, 'tp'), P(None, 'tp'), P(None, 'tp'), P('tp', None), P(None), cache_spec, cache_spec),
                         out_specs=(P('dp', None), cache_spec, cache_spec), check_vma=False)
```

```python
import functools

import jax
import jax.numpy as jnp
from jax import lax
from jax.experimental import pallas as pl
from jax.experimental.pallas import tpu as pltpu
from jax.sharding import PartitionSpec as P

SOFT_CAP = 50.0
ROPE_BASE = 10000.0
NORM_EPS = 1e-6
NEG_FILL = -1e30
MESH = pl.DeviceIdType.MESH
RING = 4


N_GATHER = 30


def comm_kernel(heads, o_ref, wo_hbm, x_hbm, wpost_hbm, out_ref,
                wo_v, x_v, wpost_ref, pair_r, comb, sp_r, scr, part, tp_r, gath,
                wo_sem, x_sem, pair_ss, pair_rs, sp_ss, sp_rs, tp_ss, tp_rs, ag_ss, ag_rs, dd_ss, dd_rs):
    y = lax.axis_index('tp')
    s = lax.axis_index('sp')
    xc = s // 2
    c = s % 2
    slab_rows, dim = comb.shape[1], comb.shape[2]
    row_block = (slab_rows - 2 * heads) // heads
    sub = row_block // RING
    width = part.shape[2]
    stat = row_block * heads

    def chip(dx, dy):
        return {'tp': (y + dy) % RING, 'sp': ((xc + dx) % RING) * 2 + c}

    partner = {'sp': xc * 2 + (1 - c)}

    barrier = pltpu.get_barrier_semaphore()
    pl.semaphore_signal(barrier, inc=1, device_id=partner, device_id_type=MESH)
    for k in range(1, RING):
        pl.semaphore_signal(barrier, inc=1, device_id=chip(k, 0), device_id_type=MESH)
        pl.semaphore_signal(barrier, inc=1, device_id=chip(0, k), device_id_type=MESH)

    wo_rows = wo_v.shape[0] // RING
    wo_copies = []
    for i in range(RING):
        rows = pl.ds(i * wo_rows, wo_rows)
        wo_copies.append(pltpu.make_async_copy(wo_hbm.at[rows], wo_v.at[rows], wo_sem.at[i]))
        wo_copies[-1].start()
    x_copy = pltpu.make_async_copy(x_hbm.at[pl.ds(pl.multiple_of(s * row_block, row_block), row_block)], x_v, x_sem.at[0])
    x_copy.start()
    gain_copy = pltpu.make_async_copy(wpost_hbm, wpost_ref, x_sem.at[1])
    gain_copy.start()

    pl.semaphore_wait(barrier, 2 * RING - 1)

    order = (2, 1, 3, 0)
    pair = []
    for k in order:
        there = (xc + k) % RING
        pair.append(pltpu.make_async_remote_copy(
            src_ref=o_ref.at[(1 - c) * RING + there], dst_ref=pair_r.at[there],
            send_sem=pair_ss.at[k], recv_sem=pair_rs.at[k], device_id=partner, device_id_type=MESH))
        pair[-1].start()
    sp_copies = {}
    for i, k in enumerate(order):
        there = (xc + k) % RING
        mine = c * RING + there
        pair[i].wait_recv()
        m0 = o_ref[mine, pl.ds(stat, heads), :]
        l0 = o_ref[mine, pl.ds(stat + heads, heads), :]
        m1 = pair_r[there, pl.ds(stat, heads), :]
        l1 = pair_r[there, pl.ds(stat + heads, heads), :]
        top = jnp.maximum(m0, m1)
        f0 = jnp.exp(m0 - top)
        f1 = jnp.exp(m1 - top)
        comb[there, pl.ds(stat, heads), :] = top
        comb[there, pl.ds(stat + heads, heads), :] = l0 * f0 + l1 * f1
        for j in range(row_block):
            rows = pl.ds(j * heads, heads)
            comb[there, rows, :] = o_ref[mine, rows, :] * f0[:, j:j + 1] + pair_r[there, rows, :] * f1[:, j:j + 1]
        if k:
            sp_copies[k] = pltpu.make_async_remote_copy(
                src_ref=comb.at[there], dst_ref=sp_r.at[RING - k - 1],
                send_sem=sp_ss.at[k - 1], recv_sem=sp_rs.at[RING - k - 1], device_id=chip(k, 0), device_id_type=MESH)
            sp_copies[k].start()

    def arrived(k):
        return pltpu.make_async_remote_copy(
            src_ref=comb.at[xc], dst_ref=sp_r.at[k - 1], send_sem=sp_ss.at[k - 1], recv_sem=sp_rs.at[k - 1],
            device_id=chip(k, 0), device_id_type=MESH)
    for k in (1, 3, 2):
        arrived(k).wait_recv()
    m_all = [comb[xc, pl.ds(stat, heads), :]] + [sp_r[k, pl.ds(stat, heads), :] for k in range(RING - 1)]
    l_all = [comb[xc, pl.ds(stat + heads, heads), :]] + [sp_r[k, pl.ds(stat + heads, heads), :] for k in range(RING - 1)]
    top = functools.reduce(jnp.maximum, m_all)
    f_all = [jnp.exp(m - top) for m in m_all]
    total = sum(l * f for l, f in zip(l_all, f_all))
    lane = lax.broadcasted_iota(jnp.int32, total.shape, 1)
    inv = 1.0 / jnp.where(lane < row_block, total, 1.0)
    f_all = [f * inv for f in f_all]
    for j in range(row_block):
        rows = pl.ds(j * heads, heads)
        acc = comb[xc, rows, :] * f_all[0][:, j:j + 1]
        for k in range(RING - 1):
            acc += sp_r[k, rows, :] * f_all[k + 1][:, j:j + 1]
        scr[rows, :] = acc
    attn = jnp.concatenate([scr[pl.ds(h, row_block, stride=heads), :].astype(jnp.bfloat16) for h in range(heads)], axis=1)

    for copy in wo_copies:
        copy.wait()
    n_chunk = tp_ss.shape[0] // (RING - 1)
    cols = width // n_chunk
    tp_copies = []
    for n in range(n_chunk):
        span = pl.ds(n * cols, cols)
        prod = jnp.dot(attn, wo_v[:, span], preferred_element_type=jnp.float32)
        for t in range(RING):
            part[t, :, span] = prod[t * sub:(t + 1) * sub]
        for k in (2, 1, 3):
            to = (y + k) % RING
            copy = pltpu.make_async_remote_copy(
                src_ref=part.at[to, :, span], dst_ref=tp_r.at[RING - k - 1, :, span],
                send_sem=tp_ss.at[n * (RING - 1) + k - 1], recv_sem=tp_rs.at[n * (RING - 1) + RING - k - 1],
                device_id=chip(0, k), device_id_type=MESH)
            copy.start()
            tp_copies.append(copy)
    x_copy.wait()
    gain_copy.wait()
    for copy in tp_copies:
        copy.wait_recv()
    ssq = jnp.zeros((sub, 1), jnp.float32)
    u_all = []
    for n in range(n_chunk):
        span = pl.ds(n * cols, cols)
        u = part[y, :, span]
        for k in range(RING - 1):
            u += tp_r[k, :, span]
        ssq += jnp.sum(u * u, axis=1, keepdims=True)
        u_all.append(u)
    scale = lax.rsqrt(ssq / width + NORM_EPS)

    a, b = xc * (1 - c) + y * c, y * (1 - c) + xc * c

    def place(da, db):
        return c * RING * RING + ((a + da) % RING) * RING + (b + db) % RING

    per = cols // dim
    for n in range(n_chunk):
        for i in range(per):
            span = pl.ds(n * cols + i * dim, dim)
            x16 = x_v[:, span].astype(jnp.float32)
            x4 = x16[0:sub]
            for t in range(1, RING):
                x4 = jnp.where(y == t, x16[t * sub:(t + 1) * sub], x4)
            gain = 1.0 + wpost_ref[n * per + i:n * per + i + 1, :]
            gath[place(0, 0), :, span] = x4 + u_all[n][:, i * dim:(i + 1) * dim] * scale * gain

    def device(da, db):
        return chip(da * (1 - c) + db * c, db * (1 - c) + da * c)

    half = width // 2
    sent = []

    def message(src, h, to, number):
        ref = gath.at[place(*src), :, pl.ds(h * half, half)]
        return pltpu.make_async_remote_copy(
            src_ref=ref, dst_ref=ref, send_sem=ag_ss.at[number], recv_sem=ag_rs.at[number],
            device_id=device(*to), device_id_type=MESH)

    def send(*args):
        copy = message(*args)
        copy.start()
        sent.append(copy)

    def wait(src, h, number):
        message(src, h, (0, 0), number).wait_recv()

    def to_pair(da, db):
        ref = gath.at[place(da, db)]
        number = da % RING * RING + db % RING
        copy = pltpu.make_async_remote_copy(
            src_ref=ref, dst_ref=ref, send_sem=dd_ss.at[number], recv_sem=dd_rs.at[number],
            device_id=partner, device_id_type=MESH)
        copy.start()
        sent.append(copy)

    sign = (1, -1)

    def first(h, d):
        send((0, 0), h, (d, 0), first_no[h, d])

    def second(da, h):
        for d in sign:
            send((da, 0), h, (0, d), second_no[da % RING, h, d])

    def got_second(da, h):
        for d in (sign[h], -sign[h]):
            wait((da, -d), h, second_no[da % RING, h, d])
            if d == sign[h]:
                send((da, -d), h, (0, d), forward_no[da % RING, h])

    def pairs(da):
        to_pair(da, -1)
        to_pair(da, 1)

    numbers = iter(range(N_GATHER))
    first_no = {(h, d): next(numbers) for h in (0, 1) for d in sign}
    diag_no = {h: next(numbers) for h in (0, 1)}
    second_no = {(k, h, d): next(numbers) for k in range(RING) for h in (0, 1) for d in sign}
    forward_no = {(k, h): next(numbers) for k in range(RING) for h in (0, 1)}

    for h in (0, 1):
        first(h, 1)
        first(h, -1)
        second(0, h)
    to_pair(0, 0)
    for h in (0, 1):
        for d in (sign[h], -sign[h]):
            wait((-d, 0), h, first_no[h, d])
            if d == sign[h]:
                send((-d, 0), h, (d, 0), diag_no[h])
            second(-d, h)
    to_pair(-1, 0)
    to_pair(1, 0)
    for h in (0, 1):
        got_second(0, h)
    pairs(0)
    for h in (0, 1):
        wait((2, 0), h, diag_no[h])
        second(2, h)
    to_pair(2, 0)
    for h in (0, 1):
        got_second(-1, h)
        got_second(1, h)
    pairs(-1)
    pairs(1)
    for h in (0, 1):
        wait((0, 2), h, forward_no[0, h])
    to_pair(0, 2)
    for h in (0, 1):
        got_second(2, h)
    pairs(2)
    for k in (-1, 1, 2):
        for h in (0, 1):
            wait((k, 2), h, forward_no[k % RING, h])
        to_pair(k, 2)

    def from_pair(da, db):
        ref = gath.at[(1 - c) * RING * RING + ((b + da) % RING) * RING + (a + db) % RING]
        number = da % RING * RING + db % RING
        pltpu.make_async_remote_copy(
            src_ref=ref, dst_ref=ref, send_sem=dd_ss.at[number], recv_sem=dd_rs.at[number],
            device_id=partner, device_id_type=MESH).wait_recv()

    def convert(kind):
        for cx in range(RING):
            rows = pl.ds(pl.multiple_of((2 * cx + kind) * row_block, row_block), row_block)
            slots = [kind * RING * RING + (1 - kind) * (cx * RING + t) + kind * (t * RING + cx) for t in range(RING)]
            for n in range(n_chunk):
                span = pl.ds(n * cols, cols)
                out_ref[rows, span] = jnp.concatenate([gath[i, :, span] for i in slots], axis=0).astype(out_ref.dtype)

    convert(c)
    for da in range(RING):
        for db in range(RING):
            from_pair(da, db)
    convert(1 - c)

    for copy in pair:
        copy.wait_send()
    for copy in list(sp_copies.values()) + tp_copies + sent:
        copy.wait_send()


def attend_kernel(kv_heads, freq_ref, pos_hbm, x_hbm, wpre_hbm, wq_hbm, wk_hbm, wv_hbm, kc_hbm, vc_hbm,
                  pack_ref, ko_hbm, vo_hbm, pos_ref, posv_ref, x_ref, wpre_ref, a_v, w_v, q_s, kn_s, vn_s, ko_ref, vo_ref, in_sem, w_sem, k_sem, v_sem, ko_sem, vo_sem):
    rows, width = x_ref.shape
    dim = pack_ref.shape[2]
    n_slab = pack_ref.shape[0]
    row_block = rows // n_slab
    heads = q_s.shape[0] // rows
    group = heads // kv_heads
    span = ko_ref.shape[1]
    seq_block = span // kv_heads
    window = kn_s.shape[0] // rows
    chunk = w_v.shape[2]
    first_pos = lax.axis_index('sp') * seq_block

    jobs = [('k', wk_hbm, i) for i in range(wk_hbm.shape[1] // chunk)]
    jobs += [('v', wv_hbm, i) for i in range(wv_hbm.shape[1] // chunk)]
    jobs += [('q', wq_hbm, i) for i in range(wq_hbm.shape[1] // chunk)]

    def w_copy(n):
        _, ref, i = jobs[n]
        return pltpu.make_async_copy(ref.at[:, pl.ds(i * chunk, chunk)], w_v.at[n], w_sem.at[n])

    def slab_copies(d):
        part = pl.ds(d * row_block, row_block)
        return (pltpu.make_async_copy(kc_hbm.at[part], ko_ref.at[part], k_sem.at[d]),
                pltpu.make_async_copy(vc_hbm.at[part], vo_ref.at[part], v_sem.at[d]))

    def out_copies(d):
        part = pl.ds(d * row_block, row_block)
        return (pltpu.make_async_copy(ko_ref.at[part], ko_hbm.at[part], ko_sem.at[d]),
                pltpu.make_async_copy(vo_ref.at[part], vo_hbm.at[part], vo_sem.at[d]))

    small = [pltpu.make_async_copy(a, b, in_sem.at[i]) for i, (a, b) in enumerate(
        ((x_hbm, x_ref), (wpre_hbm, wpre_ref), (pos_hbm, pos_ref), (pos_hbm, posv_ref)))]
    for copy in small:
        copy.start()
    w_copy(0).start()
    for copy in small:
        copy.wait()
    for n in range(1, len(jobs)):
        w_copy(n).start()

    @pl.loop(0, rows // 16)
    def _(i):
        part = pl.ds(pl.multiple_of(i * 16, 16), 16)
        squares = jnp.zeros((16, dim), jnp.float32)
        for n in range(width // dim):
            xf = x_ref[part, pl.ds(n * dim, dim)].astype(jnp.float32)
            squares += xf * xf
        scale = lax.rsqrt(jnp.sum(squares, axis=1, keepdims=True) / width + NORM_EPS)
        for n in range(width // dim):
            cols = pl.ds(n * dim, dim)
            xf = x_ref[part, cols].astype(jnp.float32)
            a_v[part, cols] = (xf * scale * (1.0 + wpre_ref[n:n + 1, :])).astype(a_v.dtype)

    half = dim // 2
    positions = jnp.broadcast_to(posv_ref[...].astype(jnp.float32), (dim, rows)).T
    angles = positions * freq_ref[0:1, :]
    cos_all = jnp.cos(angles)
    sin_all = jnp.sin(angles)
    sin_all = jnp.where(lax.broadcasted_iota(jnp.int32, sin_all.shape, 1) < half, -sin_all, sin_all)
    slabs_started = 0
    for n, (kind, _, i) in enumerate(jobs):
        w_copy(n).wait()
        upto = n_slab * (n + 1) // len(jobs)
        for d in range(slabs_started, upto):
            for copy in slab_copies(d):
                copy.start()
        slabs_started = upto
        prod = jnp.dot(a_v[...], w_v[n], preferred_element_type=jnp.float32)
        for h in range(chunk // dim):
            val = prod[:, h * dim:(h + 1) * dim]
            if kind != 'v':
                val = val * cos_all + pltpu.roll(val, half, 1) * sin_all
            head = i * (chunk // dim) + h
            if kind == 'q':
                q_s[pl.ds(head, rows, stride=heads), :] = val
            else:
                for r in range(window // kv_heads):
                    (kn_s if kind == 'k' else vn_s)[pl.ds(r * kv_heads + head, rows, stride=window), :] = val

    col = lax.broadcasted_iota(jnp.int32, (heads, span), 1)
    row = lax.broadcasted_iota(jnp.int32, (heads, span), 0)
    same_head = col % kv_heads == row // group
    lane = lax.broadcasted_iota(jnp.int32, (heads, dim), 1)
    win_time = lax.broadcasted_iota(jnp.int32, (window, dim), 0) // kv_heads
    per_window = window // kv_heads

    @pl.loop(0, n_slab)
    def _(d):
        for copy in slab_copies(d):
            copy.wait()
        last = []
        for j in range(row_block):
            b = d * row_block + j
            here = pos_ref[0, b] - first_pos
            last.append(here)
            slot = jnp.clip(here, 0, seq_block - 1)
            at = pl.ds(pl.multiple_of(slot // per_window * window, window), window)
            hit = win_time == jnp.where(here == slot, slot % per_window, -1)
            new = pl.ds(pl.multiple_of(b * window, window), window)
            ko_ref[b, at, :] = jnp.where(hit, kn_s[new, :], ko_ref[b, at, :].astype(jnp.float32)).astype(ko_ref.dtype)
            vo_ref[b, at, :] = jnp.where(hit, vn_s[new, :], vo_ref[b, at, :].astype(jnp.float32)).astype(vo_ref.dtype)
        for copy in out_copies(d):
            copy.start()
        scores = []
        for j in range(row_block):
            b = d * row_block + j
            q_b = q_s[pl.ds(pl.multiple_of(b * heads, heads), heads), :].astype(jnp.bfloat16)
            scores.append(lax.dot_general(q_b, ko_ref[b], (((1,), (1,)), ((), ())), preferred_element_type=jnp.float32))
        tops = jnp.zeros((heads, dim), jnp.float32)
        sums = jnp.zeros((heads, dim), jnp.float32)
        weights = []
        for j in range(row_block):
            valid = same_head & (col < (last[j] + 1) * kv_heads)
            capped = jnp.where(valid, SOFT_CAP * jnp.tanh(scores[j] * (dim ** -0.5 / SOFT_CAP)), NEG_FILL)
            top = jnp.max(capped, axis=1, keepdims=True)
            exp_w = jnp.where(valid, jnp.exp(capped - top), 0.0)
            tops = jnp.where(lane == j, top, tops)
            sums = jnp.where(lane == j, jnp.sum(exp_w, axis=1, keepdims=True), sums)
            weights.append(exp_w.astype(jnp.bfloat16))
        slab = d % 2 * (n_slab // 2) + d // 2
        for j in range(row_block):
            b = d * row_block + j
            pack_ref[slab, pl.ds(j * heads, heads), :] = jnp.dot(weights[j], vo_ref[b], preferred_element_type=jnp.float32)
        pack_ref[slab, pl.ds(row_block * heads, heads), :] = tops
        pack_ref[slab, pl.ds((row_block + 1) * heads, heads), :] = sums

    for d in range(n_slab):
        for copy in out_copies(d):
            copy.wait()


def in_hbm(operand):
    return pltpu.with_memory_space_constraint(operand, pltpu.HBM)


def attend(x_in, cur_pos, w_pre, w_q, w_k, w_v, k_cache, v_cache, n_sp):
    rows, seq_block, kv_heads, dim = k_cache.shape
    width = x_in.shape[1]
    heads = w_q.shape[1] // dim
    chunk = 2 * dim
    window = 16
    n_jobs = (w_q.shape[1] + w_k.shape[1] + w_v.shape[1]) // chunk
    inv_freq = ROPE_BASE ** (-2.0 * jnp.arange(dim // 2, dtype=jnp.float32) / dim)
    freq = jnp.broadcast_to(jnp.concatenate([inv_freq, inv_freq])[None], (8, dim))
    flat = (rows, seq_block * kv_heads, dim)
    sems = pltpu.SemaphoreType.DMA
    vmem = pl.BlockSpec(memory_space=pltpu.VMEM)
    hbm = pl.BlockSpec(memory_space=pltpu.HBM)
    pack, k_out, v_out = pl.pallas_call(
        functools.partial(attend_kernel, kv_heads),
        out_shape=(jax.ShapeDtypeStruct((n_sp, rows // n_sp * heads + 2 * heads, dim), jnp.float32),
                   jax.ShapeDtypeStruct(flat, k_cache.dtype), jax.ShapeDtypeStruct(flat, v_cache.dtype)),
        in_specs=[vmem] + [hbm] * 8,
        out_specs=(vmem, hbm, hbm),
        scratch_shapes=[
            pltpu.SMEM((1, rows), cur_pos.dtype),
            pltpu.VMEM((1, rows), cur_pos.dtype),
            pltpu.VMEM((rows, width), x_in.dtype),
            pltpu.VMEM((width // dim, dim), jnp.float32),
            pltpu.VMEM((rows, width), jnp.bfloat16),
            pltpu.VMEM((n_jobs, width, chunk), w_q.dtype),
            pltpu.VMEM(((rows + 1) * heads, dim), jnp.float32),
            pltpu.VMEM(((rows + 1) * window, dim), jnp.float32),
            pltpu.VMEM(((rows + 1) * window, dim), jnp.float32),
            pltpu.VMEM(flat, k_cache.dtype),
            pltpu.VMEM(flat, v_cache.dtype),
            sems((4,)), sems((n_jobs,)), sems((n_sp,)), sems((n_sp,)), sems((n_sp,)), sems((n_sp,)),
        ],
        compiler_params=pltpu.CompilerParams(vmem_limit_bytes=48 * 2**20),
        cost_estimate=pl.CostEstimate(flops=2 * rows * w_q.size * 2, bytes_accessed=w_q.size * 4 + k_cache.size * 4, transcendentals=0),
        name='attend',
    )(freq, in_hbm(cur_pos[None]), in_hbm(x_in), in_hbm(w_pre.reshape(-1, dim)),
      in_hbm(w_q), in_hbm(w_k), in_hbm(w_v), in_hbm(k_cache.reshape(flat)), in_hbm(v_cache.reshape(flat)))
    return pack, k_out.reshape(k_cache.shape), v_out.reshape(v_cache.shape)


def finish(o_pack, w_o, x_in, w_post, heads):
    rows, width = x_in.shape
    _, slab_rows, dim = o_pack.shape
    row_block = rows // (2 * RING)
    n_chunk = 3 if width % (3 * 256) == 0 else 1
    sems = pltpu.SemaphoreType.DMA
    vmem = pl.BlockSpec(memory_space=pltpu.VMEM)
    hbm = pl.BlockSpec(memory_space=pltpu.HBM)
    return pl.pallas_call(
        functools.partial(comm_kernel, heads),
        out_shape=jax.ShapeDtypeStruct((rows, width), x_in.dtype),
        in_specs=[vmem, hbm, hbm, hbm],
        out_specs=vmem,
        scratch_shapes=[
            pltpu.VMEM(w_o.shape, w_o.dtype),
            pltpu.VMEM((row_block, width), x_in.dtype),
            pltpu.VMEM((width // dim, dim), jnp.float32),
            pltpu.VMEM((RING, slab_rows, dim), jnp.float32),
            pltpu.VMEM((RING, slab_rows, dim), jnp.float32),
            pltpu.VMEM((RING - 1, slab_rows, dim), jnp.float32),
            pltpu.VMEM(((row_block + 1) * heads, dim), jnp.float32),
            pltpu.VMEM((RING, row_block // RING, width), jnp.float32),
            pltpu.VMEM((RING - 1, row_block // RING, width), jnp.float32),
            pltpu.VMEM((2 * RING * RING, row_block // RING, width), jnp.float32),
            sems((RING,)), sems((2,)),
            sems((RING,)), sems((RING,)),
            sems((RING - 1,)), sems((RING - 1,)),
            sems((n_chunk * (RING - 1),)), sems((n_chunk * (RING - 1),)),
            sems((N_GATHER,)), sems((N_GATHER,)),
            sems((RING * RING,)), sems((RING * RING,)),
        ],
        compiler_params=pltpu.CompilerParams(collective_id=0, has_side_effects=True, vmem_limit_bytes=22 * 2**20),
        cost_estimate=pl.CostEstimate(flops=2 * rows * w_o.size // 8, bytes_accessed=w_o.size * 2, transcendentals=0),
        name='finish',
    )(o_pack, in_hbm(w_o), in_hbm(x_in), in_hbm(w_post.reshape(-1, dim)))


def solution(mesh):
    cache_spec = P('dp', 'sp', 'tp', None)
    n_sp = mesh.shape['sp']
    assert n_sp == 2 * RING and mesh.shape['tp'] == RING

    def local_step(x_in, cur_pos, w_pre, w_q, w_k, w_v, w_o, w_post, k_cache, v_cache):
        heads_local = w_q.shape[1] // k_cache.shape[3]
        slabs, k_out, v_out = attend(x_in, cur_pos, w_pre, w_q, w_k, w_v, k_cache, v_cache, n_sp)
        x_out = finish(slabs, w_o, x_in, w_post, heads_local)
        return x_out, k_out, v_out

    return jax.shard_map(local_step, mesh=mesh,
                         in_specs=(P('dp', None), P('dp'), P(None), P(None, 'tp'), P(None, 'tp'), P(None, 'tp'), P('tp', None), P(None), cache_spec, cache_spec),
                         out_specs=(P('dp', None), cache_spec, cache_spec), check_vma=False)
```

```python
import functools

import jax
import jax.numpy as jnp
from jax import lax
from jax.experimental import pallas as pl
from jax.experimental.pallas import tpu as pltpu
from jax.sharding import PartitionSpec as P

SOFT_CAP = 50.0
ROPE_BASE = 10000.0
NORM_EPS = 1e-6
NEG_FILL = -1e30
MESH = pl.DeviceIdType.MESH
RING = 4


GROUPS = 2
N_GATHER = 30


def comm_kernel(heads, o_ref, wo_hbm, x_hbm, wpost_hbm, out_ref,
                wo_v, x_v, wpost_ref, pair_r, comb, sp_r, scr, part, tp_r, gath,
                wo_sem, x_sem, pair_ss, pair_rs, sp_ss, sp_rs, tp_ss, tp_rs, ag_ss, ag_rs, dd_ss, dd_rs):
    y = lax.axis_index('tp')
    s = lax.axis_index('sp')
    xc = s // 2
    c = s % 2
    slab_rows, dim = comb.shape[1], comb.shape[2]
    row_block = slab_rows // heads - 2
    group_rows = row_block // GROUPS
    sub = group_rows // RING
    width = part.shape[3]

    def chip(dx, dy):
        return {'tp': (y + dy) % RING, 'sp': ((xc + dx) % RING) * 2 + c}

    partner = {'sp': xc * 2 + (1 - c)}

    barrier = pltpu.get_barrier_semaphore()
    pl.semaphore_signal(barrier, inc=1, device_id=partner, device_id_type=MESH)
    for k in range(1, RING):
        pl.semaphore_signal(barrier, inc=1, device_id=chip(k, 0), device_id_type=MESH)
        pl.semaphore_signal(barrier, inc=1, device_id=chip(0, k), device_id_type=MESH)

    wo_rows = wo_v.shape[0] // RING
    wo_copies = []
    for i in range(RING):
        rows = pl.ds(i * wo_rows, wo_rows)
        wo_copies.append(pltpu.make_async_copy(wo_hbm.at[rows], wo_v.at[rows], wo_sem.at[i]))
        wo_copies[-1].start()
    x_copy = pltpu.make_async_copy(x_hbm.at[pl.ds(pl.multiple_of(s * row_block, row_block), row_block)], x_v, x_sem.at[0])
    x_copy.start()
    gain_copy = pltpu.make_async_copy(wpost_hbm, wpost_ref, x_sem.at[1])
    gain_copy.start()

    pl.semaphore_wait(barrier, 2 * RING - 1)
    sent = []

    def rows_of(g):
        start = (2 + g * group_rows) * heads if g else 0
        return pl.ds(start, (2 + (g + 1) * group_rows) * heads - start)

    order = (2, 1, 3, 0)
    pair = {}
    for g in range(GROUPS):
        for k in order:
            there = (xc + k) % RING
            pair[g, k] = pltpu.make_async_remote_copy(
                src_ref=o_ref.at[(1 - c) * RING + there, rows_of(g)], dst_ref=pair_r.at[there, rows_of(g)],
                send_sem=pair_ss.at[g * RING + k], recv_sem=pair_rs.at[g * RING + k], device_id=partner, device_id_type=MESH)
            pair[g, k].start()
            sent.append(pair[g, k])
    factors = {}
    for g in range(GROUPS):
        for k in order:
            there = (xc + k) % RING
            mine = c * RING + there
            pair[g, k].wait_recv()
            if g == 0:
                m0 = o_ref[mine, pl.ds(0, heads), :]
                l0 = o_ref[mine, pl.ds(heads, heads), :]
                m1 = pair_r[there, pl.ds(0, heads), :]
                l1 = pair_r[there, pl.ds(heads, heads), :]
                top = jnp.maximum(m0, m1)
                factors[k] = jnp.exp(m0 - top), jnp.exp(m1 - top)
                comb[there, pl.ds(0, heads), :] = top
                comb[there, pl.ds(heads, heads), :] = l0 * factors[k][0] + l1 * factors[k][1]
            f0, f1 = factors[k]
            for j in range(g * group_rows, (g + 1) * group_rows):
                rows = pl.ds((2 + j) * heads, heads)
                comb[there, rows, :] = o_ref[mine, rows, :] * f0[:, j:j + 1] + pair_r[there, rows, :] * f1[:, j:j + 1]
            if k:
                slot = g * (RING - 1) + RING - k - 1
                copy = pltpu.make_async_remote_copy(
                    src_ref=comb.at[there, rows_of(g)], dst_ref=sp_r.at[RING - k - 1, rows_of(g)],
                    send_sem=sp_ss.at[g * (RING - 1) + k - 1], recv_sem=sp_rs.at[slot], device_id=chip(k, 0), device_id_type=MESH)
                copy.start()
                sent.append(copy)

    n_chunk = tp_ss.shape[0] // (GROUPS * (RING - 1))
    cols = width // n_chunk
    tp_copies = {g: [] for g in range(GROUPS)}
    f_all = None
    for g in range(GROUPS):
        for k in (1, 3, 2):
            pltpu.make_async_remote_copy(
                src_ref=comb.at[xc, rows_of(g)], dst_ref=sp_r.at[k - 1, rows_of(g)],
                send_sem=sp_ss.at[g * (RING - 1) + k - 1], recv_sem=sp_rs.at[g * (RING - 1) + k - 1],
                device_id=chip(k, 0), device_id_type=MESH).wait_recv()
        if g == 0:
            m_all = [comb[xc, pl.ds(0, heads), :]] + [sp_r[k, pl.ds(0, heads), :] for k in range(RING - 1)]
            l_all = [comb[xc, pl.ds(heads, heads), :]] + [sp_r[k, pl.ds(heads, heads), :] for k in range(RING - 1)]
            top = functools.reduce(jnp.maximum, m_all)
            f_all = [jnp.exp(m - top) for m in m_all]
            total = sum(l * f for l, f in zip(l_all, f_all))
            lane = lax.broadcasted_iota(jnp.int32, total.shape, 1)
            inv = 1.0 / jnp.where(lane < row_block, total, 1.0)
            f_all = [f * inv for f in f_all]
        for j in range(group_rows):
            row = g * group_rows + j
            rows = pl.ds((2 + row) * heads, heads)
            acc = comb[xc, rows, :] * f_all[0][:, row:row + 1]
            for k in range(RING - 1):
                acc += sp_r[k, rows, :] * f_all[k + 1][:, row:row + 1]
            scr[g, pl.ds(j * heads, heads), :] = acc
        attn = jnp.concatenate([scr[g, pl.ds(h, group_rows, stride=heads), :].astype(jnp.bfloat16) for h in range(heads)], axis=1)
        if g == 0:
            for copy in wo_copies:
                copy.wait()
        for n in range(n_chunk):
            span = pl.ds(n * cols, cols)
            prod = jnp.dot(attn, wo_v[:, span], preferred_element_type=jnp.float32)
            for t in range(RING):
                part[g, t, :, span] = prod[t * sub:(t + 1) * sub]
            for k in (2, 1, 3):
                to = (y + k) % RING
                number = (g * n_chunk + n) * (RING - 1)
                copy = pltpu.make_async_remote_copy(
                    src_ref=part.at[g, to, :, span], dst_ref=tp_r.at[g, RING - k - 1, :, span],
                    send_sem=tp_ss.at[number + k - 1], recv_sem=tp_rs.at[number + RING - k - 1],
                    device_id=chip(0, k), device_id_type=MESH)
                copy.start()
                tp_copies[g].append(copy)
                sent.append(copy)
    x_copy.wait()
    gain_copy.wait()

    a, b = xc * (1 - c) + y * c, y * (1 - c) + xc * c

    def place(da, db):
        return c * RING * RING + ((a + da) % RING) * RING + (b + db) % RING

    def device(da, db):
        return chip(da * (1 - c) + db * c, db * (1 - c) + da * c)

    def normalise(g):
        for copy in tp_copies[g]:
            copy.wait_recv()
        squares = jnp.zeros((sub, dim), jnp.float32)
        u_all = []
        for n in range(width // dim):
            span = pl.ds(n * dim, dim)
            u = part[g, y, :, span]
            for k in range(RING - 1):
                u += tp_r[g, k, :, span]
            squares += u * u
            u_all.append(u)
        scale = lax.rsqrt(jnp.sum(squares, axis=1, keepdims=True) / width + NORM_EPS)
        for n in range(width // dim):
            span = pl.ds(n * dim, dim)
            x_group = x_v[:, span].astype(jnp.float32)[g * group_rows:(g + 1) * group_rows]
            x_own = x_group[0:sub]
            for t in range(1, RING):
                x_own = jnp.where(y == t, x_group[t * sub:(t + 1) * sub], x_own)
            gath[g, place(0, 0), :, span] = x_own + u_all[n] * scale * (1.0 + wpost_ref[n:n + 1, :])

    def message(src, g, to, number):
        ref = gath.at[g, place(*src)]
        return pltpu.make_async_remote_copy(
            src_ref=ref, dst_ref=ref, send_sem=ag_ss.at[number], recv_sem=ag_rs.at[number],
            device_id=device(*to), device_id_type=MESH)

    def send(*args):
        copy = message(*args)
        copy.start()
        sent.append(copy)

    def wait(src, g, number):
        message(src, g, (0, 0), number).wait_recv()

    def to_pair(da, db, g):
        ref = gath.at[g, place(da, db)]
        number = (g * RING + da % RING) * RING + db % RING
        copy = pltpu.make_async_remote_copy(
            src_ref=ref, dst_ref=ref, send_sem=dd_ss.at[number], recv_sem=dd_rs.at[number],
            device_id=partner, device_id_type=MESH)
        copy.start()
        sent.append(copy)

    sign = (1, -1)
    numbers = iter(range(N_GATHER))
    first_no = {(g, d): next(numbers) for g in (0, 1) for d in sign}
    diag_no = {g: next(numbers) for g in (0, 1)}
    second_no = {(k, g, d): next(numbers) for k in range(RING) for g in (0, 1) for d in sign}
    forward_no = {(k, g): next(numbers) for k in range(RING) for g in (0, 1)}

    def second(da, g):
        for d in sign:
            send((da, 0), g, (0, d), second_no[da % RING, g, d])

    def got_second(da, g):
        for d in (sign[g], -sign[g]):
            wait((da, -d), g, second_no[da % RING, g, d])
            if d == sign[g]:
                send((da, -d), g, (0, d), forward_no[da % RING, g])
            to_pair(da, -d, g)

    def got_forward(da, g):
        wait((da, 2), g, forward_no[da % RING, g])
        to_pair(da, 2, g)

    def step_start(g):
        for d in (sign[g], -sign[g]):
            send((0, 0), g, (d, 0), first_no[g, d])
        second(0, g)
        to_pair(0, 0, g)

    def step_first(g):
        for d in (sign[g], -sign[g]):
            wait((-d, 0), g, first_no[g, d])
            if d == sign[g]:
                send((-d, 0), g, (d, 0), diag_no[g])
            second(-d, g)
            to_pair(-d, 0, g)

    def step_own(g):
        got_second(0, g)

    def step_diag(g):
        wait((2, 0), g, diag_no[g])
        second(2, g)
        to_pair(2, 0, g)

    def step_sides(g):
        got_second(-sign[g], g)
        got_second(sign[g], g)

    def step_last(g):
        got_forward(0, g)
        got_second(2, g)

    def step_end(g):
        for k in (-sign[g], sign[g], 2):
            got_forward(k, g)

    def convert(kind, g):
        for cx in range(RING):
            rows = pl.ds(pl.multiple_of((2 * cx + kind) * row_block + g * group_rows, group_rows), group_rows)
            slots = [kind * RING * RING + (1 - kind) * (cx * RING + t) + kind * (t * RING + cx) for t in range(RING)]
            for n in range(n_chunk):
                span = pl.ds(n * cols, cols)
                out_ref[rows, span] = jnp.concatenate([gath[g, i, :, span] for i in slots], axis=0).astype(out_ref.dtype)

    def from_pair(g):
        for da in range(RING):
            for db in range(RING):
                ref = gath.at[g, (1 - c) * RING * RING + ((b + da) % RING) * RING + (a + db) % RING]
                number = (g * RING + da) * RING + db
                pltpu.make_async_remote_copy(
                    src_ref=ref, dst_ref=ref, send_sem=dd_ss.at[number], recv_sem=dd_rs.at[number],
                    device_id=partner, device_id_type=MESH).wait_recv()

    normalise(0)
    step_start(0)
    normalise(1)
    step_start(1)
    step_first(0)
    step_own(0)
    step_diag(0)
    step_first(1)
    step_sides(0)
    step_own(1)
    step_diag(1)
    step_last(0)
    step_sides(1)
    step_end(0)
    step_last(1)
    step_end(1)
    convert(c, 0)
    from_pair(0)
    convert(1 - c, 0)
    convert(c, 1)
    from_pair(1)
    convert(1 - c, 1)

    for copy in sent:
        copy.wait_send()


def attend_kernel(kv_heads, freq_ref, pos_hbm, x_hbm, wpre_hbm, wq_hbm, wk_hbm, wv_hbm, kc_hbm, vc_hbm,
                  pack_ref, ko_hbm, vo_hbm, pos_ref, posv_ref, x_ref, wpre_ref, a_v, w_v, q_s, kn_s, vn_s, ko_ref, vo_ref, in_sem, w_sem, k_sem, v_sem, ko_sem, vo_sem):
    rows, width = x_ref.shape
    dim = pack_ref.shape[2]
    n_slab = pack_ref.shape[0]
    row_block = rows // n_slab
    heads = q_s.shape[0] // rows
    group = heads // kv_heads
    span = ko_ref.shape[1]
    seq_block = span // kv_heads
    window = kn_s.shape[0] // rows
    chunk = w_v.shape[2]
    first_pos = lax.axis_index('sp') * seq_block

    jobs = [('k', wk_hbm, i) for i in range(wk_hbm.shape[1] // chunk)]
    jobs += [('v', wv_hbm, i) for i in range(wv_hbm.shape[1] // chunk)]
    jobs += [('q', wq_hbm, i) for i in range(wq_hbm.shape[1] // chunk)]

    def w_copy(n):
        _, ref, i = jobs[n]
        return pltpu.make_async_copy(ref.at[:, pl.ds(i * chunk, chunk)], w_v.at[n], w_sem.at[n])

    def slab_copies(d):
        part = pl.ds(d * row_block, row_block)
        return (pltpu.make_async_copy(kc_hbm.at[part], ko_ref.at[part], k_sem.at[d]),
                pltpu.make_async_copy(vc_hbm.at[part], vo_ref.at[part], v_sem.at[d]))

    def out_copies(d):
        part = pl.ds(d * row_block, row_block)
        return (pltpu.make_async_copy(ko_ref.at[part], ko_hbm.at[part], ko_sem.at[d]),
                pltpu.make_async_copy(vo_ref.at[part], vo_hbm.at[part], vo_sem.at[d]))

    small = [pltpu.make_async_copy(a, b, in_sem.at[i]) for i, (a, b) in enumerate(
        ((x_hbm, x_ref), (wpre_hbm, wpre_ref), (pos_hbm, pos_ref), (pos_hbm, posv_ref)))]
    for copy in small:
        copy.start()
    w_copy(0).start()
    for copy in small:
        copy.wait()
    for n in range(1, len(jobs)):
        w_copy(n).start()

    @pl.loop(0, rows // 16)
    def _(i):
        part = pl.ds(pl.multiple_of(i * 16, 16), 16)
        squares = jnp.zeros((16, dim), jnp.float32)
        for n in range(width // dim):
            xf = x_ref[part, pl.ds(n * dim, dim)].astype(jnp.float32)
            squares += xf * xf
        scale = lax.rsqrt(jnp.sum(squares, axis=1, keepdims=True) / width + NORM_EPS)
        for n in range(width // dim):
            cols = pl.ds(n * dim, dim)
            xf = x_ref[part, cols].astype(jnp.float32)
            a_v[part, cols] = (xf * scale * (1.0 + wpre_ref[n:n + 1, :])).astype(a_v.dtype)

    half = dim // 2
    positions = jnp.broadcast_to(posv_ref[...].astype(jnp.float32), (dim, rows)).T
    angles = positions * freq_ref[0:1, :]
    cos_all = jnp.cos(angles)
    sin_all = jnp.sin(angles)
    sin_all = jnp.where(lax.broadcasted_iota(jnp.int32, sin_all.shape, 1) < half, -sin_all, sin_all)
    slabs_started = 0
    for n, (kind, _, i) in enumerate(jobs):
        w_copy(n).wait()
        upto = n_slab * (n + 1) // len(jobs)
        for d in range(slabs_started, upto):
            for copy in slab_copies(d):
                copy.start()
        slabs_started = upto
        prod = jnp.dot(a_v[...], w_v[n], preferred_element_type=jnp.float32)
        for h in range(chunk // dim):
            val = prod[:, h * dim:(h + 1) * dim]
            if kind != 'v':
                val = val * cos_all + pltpu.roll(val, half, 1) * sin_all
            head = i * (chunk // dim) + h
            if kind == 'q':
                q_s[pl.ds(head, rows, stride=heads), :] = val
            else:
                for r in range(window // kv_heads):
                    (kn_s if kind == 'k' else vn_s)[pl.ds(r * kv_heads + head, rows, stride=window), :] = val

    col = lax.broadcasted_iota(jnp.int32, (heads, span), 1)
    row = lax.broadcasted_iota(jnp.int32, (heads, span), 0)
    same_head = col % kv_heads == row // group
    lane = lax.broadcasted_iota(jnp.int32, (heads, dim), 1)
    win_time = lax.broadcasted_iota(jnp.int32, (window, dim), 0) // kv_heads
    per_window = window // kv_heads

    @pl.loop(0, n_slab)
    def _(d):
        for copy in slab_copies(d):
            copy.wait()
        last = []
        for j in range(row_block):
            b = d * row_block + j
            here = pos_ref[0, b] - first_pos
            last.append(here)
            slot = jnp.clip(here, 0, seq_block - 1)
            at = pl.ds(pl.multiple_of(slot // per_window * window, window), window)
            hit = win_time == jnp.where(here == slot, slot % per_window, -1)
            new = pl.ds(pl.multiple_of(b * window, window), window)
            ko_ref[b, at, :] = jnp.where(hit, kn_s[new, :], ko_ref[b, at, :].astype(jnp.float32)).astype(ko_ref.dtype)
            vo_ref[b, at, :] = jnp.where(hit, vn_s[new, :], vo_ref[b, at, :].astype(jnp.float32)).astype(vo_ref.dtype)
        for copy in out_copies(d):
            copy.start()
        scores = []
        for j in range(row_block):
            b = d * row_block + j
            q_b = q_s[pl.ds(pl.multiple_of(b * heads, heads), heads), :].astype(jnp.bfloat16)
            scores.append(lax.dot_general(q_b, ko_ref[b], (((1,), (1,)), ((), ())), preferred_element_type=jnp.float32))
        tops = jnp.zeros((heads, dim), jnp.float32)
        sums = jnp.zeros((heads, dim), jnp.float32)
        weights = []
        for j in range(row_block):
            valid = same_head & (col < (last[j] + 1) * kv_heads)
            capped = jnp.where(valid, SOFT_CAP * jnp.tanh(scores[j] * (dim ** -0.5 / SOFT_CAP)), NEG_FILL)
            top = jnp.max(capped, axis=1, keepdims=True)
            exp_w = jnp.where(valid, jnp.exp(capped - top), 0.0)
            tops = jnp.where(lane == j, top, tops)
            sums = jnp.where(lane == j, jnp.sum(exp_w, axis=1, keepdims=True), sums)
            weights.append(exp_w.astype(jnp.bfloat16))
        slab = d % 2 * (n_slab // 2) + d // 2
        for j in range(row_block):
            b = d * row_block + j
            pack_ref[slab, pl.ds((j + 2) * heads, heads), :] = jnp.dot(weights[j], vo_ref[b], preferred_element_type=jnp.float32)
        pack_ref[slab, pl.ds(0, heads), :] = tops
        pack_ref[slab, pl.ds(heads, heads), :] = sums

    for d in range(n_slab):
        for copy in out_copies(d):
            copy.wait()


def in_hbm(operand):
    return pltpu.with_memory_space_constraint(operand, pltpu.HBM)


def attend(x_in, cur_pos, w_pre, w_q, w_k, w_v, k_cache, v_cache, n_sp):
    rows, seq_block, kv_heads, dim = k_cache.shape
    width = x_in.shape[1]
    heads = w_q.shape[1] // dim
    chunk = 2 * dim
    window = 16
    n_jobs = (w_q.shape[1] + w_k.shape[1] + w_v.shape[1]) // chunk
    inv_freq = ROPE_BASE ** (-2.0 * jnp.arange(dim // 2, dtype=jnp.float32) / dim)
    freq = jnp.broadcast_to(jnp.concatenate([inv_freq, inv_freq])[None], (8, dim))
    flat = (rows, seq_block * kv_heads, dim)
    sems = pltpu.SemaphoreType.DMA
    vmem = pl.BlockSpec(memory_space=pltpu.VMEM)
    hbm = pl.BlockSpec(memory_space=pltpu.HBM)
    pack, k_out, v_out = pl.pallas_call(
        functools.partial(attend_kernel, kv_heads),
        out_shape=(jax.ShapeDtypeStruct((n_sp, rows // n_sp * heads + 2 * heads, dim), jnp.float32),
                   jax.ShapeDtypeStruct(flat, k_cache.dtype), jax.ShapeDtypeStruct(flat, v_cache.dtype)),
        in_specs=[vmem] + [hbm] * 8,
        out_specs=(vmem, hbm, hbm),
        scratch_shapes=[
            pltpu.SMEM((1, rows), cur_pos.dtype),
            pltpu.VMEM((1, rows), cur_pos.dtype),
            pltpu.VMEM((rows, width), x_in.dtype),
            pltpu.VMEM((width // dim, dim), jnp.float32),
            pltpu.VMEM((rows, width), jnp.bfloat16),
            pltpu.VMEM((n_jobs, width, chunk), w_q.dtype),
            pltpu.VMEM(((rows + 1) * heads, dim), jnp.float32),
            pltpu.VMEM(((rows + 1) * window, dim), jnp.float32),
            pltpu.VMEM(((rows + 1) * window, dim), jnp.float32),
            pltpu.VMEM(flat, k_cache.dtype),
            pltpu.VMEM(flat, v_cache.dtype),
            sems((4,)), sems((n_jobs,)), sems((n_sp,)), sems((n_sp,)), sems((n_sp,)), sems((n_sp,)),
        ],
        compiler_params=pltpu.CompilerParams(vmem_limit_bytes=48 * 2**20),
        cost_estimate=pl.CostEstimate(flops=2 * rows * w_q.size * 2, bytes_accessed=w_q.size * 4 + k_cache.size * 4, transcendentals=0),
        name='attend',
    )(freq, in_hbm(cur_pos[None]), in_hbm(x_in), in_hbm(w_pre.reshape(-1, dim)),
      in_hbm(w_q), in_hbm(w_k), in_hbm(w_v), in_hbm(k_cache.reshape(flat)), in_hbm(v_cache.reshape(flat)))
    return pack, k_out.reshape(k_cache.shape), v_out.reshape(v_cache.shape)


def finish(o_pack, w_o, x_in, w_post, heads):
    rows, width = x_in.shape
    _, slab_rows, dim = o_pack.shape
    row_block = rows // (2 * RING)
    sub = row_block // (GROUPS * RING)
    n_chunk = 3 if width % (3 * 256) == 0 else 1
    sems = pltpu.SemaphoreType.DMA
    vmem = pl.BlockSpec(memory_space=pltpu.VMEM)
    hbm = pl.BlockSpec(memory_space=pltpu.HBM)
    return pl.pallas_call(
        functools.partial(comm_kernel, heads),
        out_shape=jax.ShapeDtypeStruct((rows, width), x_in.dtype),
        in_specs=[vmem, hbm, hbm, hbm],
        out_specs=vmem,
        scratch_shapes=[
            pltpu.VMEM(w_o.shape, w_o.dtype),
            pltpu.VMEM((row_block, width), x_in.dtype),
            pltpu.VMEM((width // dim, dim), jnp.float32),
            pltpu.VMEM((RING, slab_rows, dim), jnp.float32),
            pltpu.VMEM((RING, slab_rows, dim), jnp.float32),
            pltpu.VMEM((RING - 1, slab_rows, dim), jnp.float32),
            pltpu.VMEM((GROUPS, (row_block // GROUPS + 1) * heads, dim), jnp.float32),
            pltpu.VMEM((GROUPS, RING, sub, width), jnp.float32),
            pltpu.VMEM((GROUPS, RING - 1, sub, width), jnp.float32),
            pltpu.VMEM((GROUPS, 2 * RING * RING, sub, width), jnp.float32),
            sems((RING,)), sems((2,)),
            sems((GROUPS * RING,)), sems((GROUPS * RING,)),
            sems((GROUPS * (RING - 1),)), sems((GROUPS * (RING - 1),)),
            sems((GROUPS * n_chunk * (RING - 1),)), sems((GROUPS * n_chunk * (RING - 1),)),
            sems((N_GATHER,)), sems((N_GATHER,)),
            sems((GROUPS * RING * RING,)), sems((GROUPS * RING * RING,)),
        ],
        compiler_params=pltpu.CompilerParams(collective_id=0, has_side_effects=True, vmem_limit_bytes=22 * 2**20),
        cost_estimate=pl.CostEstimate(flops=2 * rows * w_o.size // 8, bytes_accessed=w_o.size * 2, transcendentals=0),
        name='finish',
    )(o_pack, in_hbm(w_o), in_hbm(x_in), in_hbm(w_post.reshape(-1, dim)))


def solution(mesh):
    cache_spec = P('dp', 'sp', 'tp', None)
    n_sp = mesh.shape['sp']
    assert n_sp == 2 * RING and mesh.shape['tp'] == RING

    def local_step(x_in, cur_pos, w_pre, w_q, w_k, w_v, w_o, w_post, k_cache, v_cache):
        heads_local = w_q.shape[1] // k_cache.shape[3]
        slabs, k_out, v_out = attend(x_in, cur_pos, w_pre, w_q, w_k, w_v, k_cache, v_cache, n_sp)
        x_out = finish(slabs, w_o, x_in, w_post, heads_local)
        return x_out, k_out, v_out

    return jax.shard_map(local_step, mesh=mesh,
                         in_specs=(P('dp', None), P('dp'), P(None), P(None, 'tp'), P(None, 'tp'), P(None, 'tp'), P('tp', None), P(None), cache_spec, cache_spec),
                         out_specs=(P('dp', None), cache_spec, cache_spec), check_vma=False)
```

```python
import functools

import jax
import jax.numpy as jnp
from jax import lax
from jax.experimental import pallas as pl
from jax.experimental.pallas import tpu as pltpu
from jax.sharding import PartitionSpec as P

SOFT_CAP = 50.0
ROPE_BASE = 10000.0
NORM_EPS = 1e-6
NEG_FILL = -1e30
MESH = pl.DeviceIdType.MESH
RING = 4


N_GATHER = 30


def comm_kernel(heads, o_ref, wo_hbm, x_hbm, wpost_hbm, out_ref,
                wo_v, x_v, wpost_ref, pair_r, comb, sp_r, scr, part, tp_r, gath,
                wo_sem, x_sem, pair_ss, pair_rs, sp_ss, sp_rs, tp_ss, tp_rs, ag_ss, ag_rs, dd_ss, dd_rs):
    y = lax.axis_index('tp')
    s = lax.axis_index('sp')
    xc = s // 2
    c = s % 2
    slab_rows, dim = comb.shape[1], comb.shape[2]
    row_block = (slab_rows - 2 * heads) // heads
    sub = row_block // RING
    width = part.shape[2]
    stat = row_block * heads

    def chip(dx, dy):
        return {'tp': (y + dy) % RING, 'sp': ((xc + dx) % RING) * 2 + c}

    partner = {'sp': xc * 2 + (1 - c)}

    barrier = pltpu.get_barrier_semaphore()
    pl.semaphore_signal(barrier, inc=1, device_id=partner, device_id_type=MESH)
    for k in range(1, RING):
        pl.semaphore_signal(barrier, inc=1, device_id=chip(k, 0), device_id_type=MESH)
        pl.semaphore_signal(barrier, inc=1, device_id=chip(0, k), device_id_type=MESH)

    wo_rows = wo_v.shape[0] // RING
    wo_copies = []
    for i in range(RING):
        rows = pl.ds(i * wo_rows, wo_rows)
        wo_copies.append(pltpu.make_async_copy(wo_hbm.at[rows], wo_v.at[rows], wo_sem.at[i]))
        wo_copies[-1].start()
    x_copy = pltpu.make_async_copy(x_hbm.at[pl.ds(pl.multiple_of(s * row_block, row_block), row_block)], x_v, x_sem.at[0])
    x_copy.start()
    gain_copy = pltpu.make_async_copy(wpost_hbm, wpost_ref, x_sem.at[1])
    gain_copy.start()

    pl.semaphore_wait(barrier, 2 * RING - 1)

    order = (2, 1, 3, 0)
    pair = []
    for k in order:
        there = (xc + k) % RING
        pair.append(pltpu.make_async_remote_copy(
            src_ref=o_ref.at[(1 - c) * RING + there], dst_ref=pair_r.at[there],
            send_sem=pair_ss.at[k], recv_sem=pair_rs.at[k], device_id=partner, device_id_type=MESH))
        pair[-1].start()
    sp_copies = {}
    for i, k in enumerate(order):
        there = (xc + k) % RING
        mine = c * RING + there
        pair[i].wait_recv()
        m0 = o_ref[mine, pl.ds(stat, heads), :]
        l0 = o_ref[mine, pl.ds(stat + heads, heads), :]
        m1 = pair_r[there, pl.ds(stat, heads), :]
        l1 = pair_r[there, pl.ds(stat + heads, heads), :]
        top = jnp.maximum(m0, m1)
        f0 = jnp.exp(m0 - top)
        f1 = jnp.exp(m1 - top)
        comb[there, pl.ds(stat, heads), :] = top
        comb[there, pl.ds(stat + heads, heads), :] = l0 * f0 + l1 * f1
        for j in range(row_block):
            rows = pl.ds(j * heads, heads)
            comb[there, rows, :] = o_ref[mine, rows, :] * f0[:, j:j + 1] + pair_r[there, rows, :] * f1[:, j:j + 1]
        if k:
            sp_copies[k] = pltpu.make_async_remote_copy(
                src_ref=comb.at[there], dst_ref=sp_r.at[RING - k - 1],
                send_sem=sp_ss.at[k - 1], recv_sem=sp_rs.at[RING - k - 1], device_id=chip(k, 0), device_id_type=MESH)
            sp_copies[k].start()

    def arrived(k):
        return pltpu.make_async_remote_copy(
            src_ref=comb.at[xc], dst_ref=sp_r.at[k - 1], send_sem=sp_ss.at[k - 1], recv_sem=sp_rs.at[k - 1],
            device_id=chip(k, 0), device_id_type=MESH)
    for k in (1, 3, 2):
        arrived(k).wait_recv()
    m_all = [comb[xc, pl.ds(stat, heads), :]] + [sp_r[k, pl.ds(stat, heads), :] for k in range(RING - 1)]
    l_all = [comb[xc, pl.ds(stat + heads, heads), :]] + [sp_r[k, pl.ds(stat + heads, heads), :] for k in range(RING - 1)]
    top = functools.reduce(jnp.maximum, m_all)
    f_all = [jnp.exp(m - top) for m in m_all]
    total = sum(l * f for l, f in zip(l_all, f_all))
    lane = lax.broadcasted_iota(jnp.int32, total.shape, 1)
    inv = 1.0 / jnp.where(lane < row_block, total, 1.0)
    f_all = [f * inv for f in f_all]
    for j in range(row_block):
        rows = pl.ds(j * heads, heads)
        acc = comb[xc, rows, :] * f_all[0][:, j:j + 1]
        for k in range(RING - 1):
            acc += sp_r[k, rows, :] * f_all[k + 1][:, j:j + 1]
        scr[rows, :] = acc
    attn = jnp.concatenate([scr[pl.ds(h, row_block, stride=heads), :].astype(jnp.bfloat16) for h in range(heads)], axis=1)

    for copy in wo_copies:
        copy.wait()
    n_chunk = tp_ss.shape[0] // (RING - 1)
    cols = width // n_chunk
    tp_copies = []
    for n in range(n_chunk):
        span = pl.ds(n * cols, cols)
        prod = jnp.dot(attn, wo_v[:, span], preferred_element_type=jnp.float32)
        for t in range(RING):
            part[t, :, span] = prod[t * sub:(t + 1) * sub]
        for k in (2, 1, 3):
            to = (y + k) % RING
            copy = pltpu.make_async_remote_copy(
                src_ref=part.at[to, :, span], dst_ref=tp_r.at[RING - k - 1, :, span],
                send_sem=tp_ss.at[n * (RING - 1) + k - 1], recv_sem=tp_rs.at[n * (RING - 1) + RING - k - 1],
                device_id=chip(0, k), device_id_type=MESH)
            copy.start()
            tp_copies.append(copy)
    x_copy.wait()
    gain_copy.wait()
    for copy in tp_copies:
        copy.wait_recv()
    ssq = jnp.zeros((sub, 1), jnp.float32)
    u_all = []
    for n in range(n_chunk):
        span = pl.ds(n * cols, cols)
        u = part[y, :, span]
        for k in range(RING - 1):
            u += tp_r[k, :, span]
        ssq += jnp.sum(u * u, axis=1, keepdims=True)
        u_all.append(u)
    scale = lax.rsqrt(ssq / width + NORM_EPS)

    a, b = xc * (1 - c) + y * c, y * (1 - c) + xc * c

    def place(da, db):
        return c * RING * RING + ((a + da) % RING) * RING + (b + db) % RING

    per = cols // dim
    for n in range(n_chunk):
        for i in range(per):
            span = pl.ds(n * cols + i * dim, dim)
            x16 = x_v[:, span].astype(jnp.float32)
            x4 = x16[0:sub]
            for t in range(1, RING):
                x4 = jnp.where(y == t, x16[t * sub:(t + 1) * sub], x4)
            gain = 1.0 + wpost_ref[n * per + i:n * per + i + 1, :]
            gath[place(0, 0), :, span] = x4 + u_all[n][:, i * dim:(i + 1) * dim] * scale * gain

    def device(da, db):
        return chip(da * (1 - c) + db * c, db * (1 - c) + da * c)

    half = width // 2
    sent = []

    def message(src, h, to, number):
        ref = gath.at[place(*src), :, pl.ds(h * half, half)]
        return pltpu.make_async_remote_copy(
            src_ref=ref, dst_ref=ref, send_sem=ag_ss.at[number], recv_sem=ag_rs.at[number],
            device_id=device(*to), device_id_type=MESH)

    def send(*args):
        copy = message(*args)
        copy.start()
        sent.append(copy)

    def wait(src, h, number):
        message(src, h, (0, 0), number).wait_recv()

    def to_pair(da, db):
        ref = gath.at[place(da, db)]
        number = da % RING * RING + db % RING
        copy = pltpu.make_async_remote_copy(
            src_ref=ref, dst_ref=ref, send_sem=dd_ss.at[number], recv_sem=dd_rs.at[number],
            device_id=partner, device_id_type=MESH)
        copy.start()
        sent.append(copy)

    sign = (1, -1)
    numbers = iter(range(N_GATHER))
    first_no = {(h, d): next(numbers) for h in (0, 1) for d in (1, -1, 2)}
    second_no = {(k, h, d): next(numbers) for k in range(RING) for h in (0, 1) for d in ((1, -1, 2) if k == 2 else sign)}
    forward_no = {(k, h): next(numbers) for k in (0, 1, 3) for h in (0, 1)}

    def second(da, h):
        for d in (2, 1, -1) if da == 2 else sign:
            send((da, 0), h, (0, d), second_no[da % RING, h, d])

    def got_second(da, h):
        for d in (sign[h], -sign[h]):
            wait((da, -d), h, second_no[da % RING, h, d])
            if da != 2 and d == sign[h]:
                send((da, -d), h, (0, d), forward_no[da % RING, h])

    def pairs(da):
        to_pair(da, -1)
        to_pair(da, 1)

    for h in (0, 1):
        for d in (2, 1, -1):
            send((0, 0), h, (d, 0), first_no[h, d])
        second(0, h)
    to_pair(0, 0)
    for h in (0, 1):
        for d in (sign[h], -sign[h]):
            wait((-d, 0), h, first_no[h, d])
            second(-d, h)
    for h in (0, 1):
        wait((2, 0), h, first_no[h, 2])
        second(2, h)
    to_pair(-1, 0)
    to_pair(1, 0)
    to_pair(2, 0)
    for h in (0, 1):
        got_second(0, h)
    pairs(0)
    for h in (0, 1):
        got_second(-1, h)
        got_second(1, h)
    pairs(-1)
    pairs(1)
    for h in (0, 1):
        wait((0, 2), h, forward_no[0, h])
    to_pair(0, 2)
    for h in (0, 1):
        got_second(2, h)
    pairs(2)
    for k in (-1, 1):
        for h in (0, 1):
            wait((k, 2), h, forward_no[k % RING, h])
        to_pair(k, 2)
    for h in (0, 1):
        wait((2, 2), h, second_no[2, h, 2])
    to_pair(2, 2)

    def from_pair(da, db):
        ref = gath.at[(1 - c) * RING * RING + ((b + da) % RING) * RING + (a + db) % RING]
        number = da % RING * RING + db % RING
        pltpu.make_async_remote_copy(
            src_ref=ref, dst_ref=ref, send_sem=dd_ss.at[number], recv_sem=dd_rs.at[number],
            device_id=partner, device_id_type=MESH).wait_recv()

    def convert(kind):
        for cx in range(RING):
            rows = pl.ds(pl.multiple_of((2 * cx + kind) * row_block, row_block), row_block)
            slots = [kind * RING * RING + (1 - kind) * (cx * RING + t) + kind * (t * RING + cx) for t in range(RING)]
            for n in range(n_chunk):
                span = pl.ds(n * cols, cols)
                out_ref[rows, span] = jnp.concatenate([gath[i, :, span] for i in slots], axis=0).astype(out_ref.dtype)

    convert(c)
    for da in range(RING):
        for db in range(RING):
            from_pair(da, db)
    convert(1 - c)

    for copy in pair:
        copy.wait_send()
    for copy in list(sp_copies.values()) + tp_copies + sent:
        copy.wait_send()


def attend_kernel(kv_heads, freq_ref, pos_hbm, x_hbm, wpre_hbm, wq_hbm, wk_hbm, wv_hbm, kc_hbm, vc_hbm,
                  pack_ref, ko_hbm, vo_hbm, pos_ref, posv_ref, x_ref, wpre_ref, a_v, w_v, q_s, kn_s, vn_s, ko_ref, vo_ref, in_sem, w_sem, k_sem, v_sem, ko_sem, vo_sem):
    rows, width = x_ref.shape
    dim = pack_ref.shape[2]
    n_slab = pack_ref.shape[0]
    row_block = rows // n_slab
    heads = q_s.shape[0] // rows
    group = heads // kv_heads
    span = ko_ref.shape[1]
    seq_block = span // kv_heads
    window = kn_s.shape[0] // rows
    chunk = w_v.shape[2]
    first_pos = lax.axis_index('sp') * seq_block

    jobs = [('k', wk_hbm, i) for i in range(wk_hbm.shape[1] // chunk)]
    jobs += [('v', wv_hbm, i) for i in range(wv_hbm.shape[1] // chunk)]
    jobs += [('q', wq_hbm, i) for i in range(wq_hbm.shape[1] // chunk)]

    def w_copy(n):
        _, ref, i = jobs[n]
        return pltpu.make_async_copy(ref.at[:, pl.ds(i * chunk, chunk)], w_v.at[n], w_sem.at[n])

    def slab_copies(d):
        part = pl.ds(d * row_block, row_block)
        return (pltpu.make_async_copy(kc_hbm.at[part], ko_ref.at[part], k_sem.at[d]),
                pltpu.make_async_copy(vc_hbm.at[part], vo_ref.at[part], v_sem.at[d]))

    def out_copies(d):
        part = pl.ds(d * row_block, row_block)
        return (pltpu.make_async_copy(ko_ref.at[part], ko_hbm.at[part], ko_sem.at[d]),
                pltpu.make_async_copy(vo_ref.at[part], vo_hbm.at[part], vo_sem.at[d]))

    small = [pltpu.make_async_copy(a, b, in_sem.at[i]) for i, (a, b) in enumerate(
        ((x_hbm, x_ref), (wpre_hbm, wpre_ref), (pos_hbm, pos_ref), (pos_hbm, posv_ref)))]
    for copy in small:
        copy.start()
    w_copy(0).start()
    for copy in small:
        copy.wait()
    for n in range(1, len(jobs)):
        w_copy(n).start()

    @pl.loop(0, rows // 16)
    def _(i):
        part = pl.ds(pl.multiple_of(i * 16, 16), 16)
        squares = jnp.zeros((16, dim), jnp.float32)
        for n in range(width // dim):
            xf = x_ref[part, pl.ds(n * dim, dim)].astype(jnp.float32)
            squares += xf * xf
        scale = lax.rsqrt(jnp.sum(squares, axis=1, keepdims=True) / width + NORM_EPS)
        for n in range(width // dim):
            cols = pl.ds(n * dim, dim)
            xf = x_ref[part, cols].astype(jnp.float32)
            a_v[part, cols] = (xf * scale * (1.0 + wpre_ref[n:n + 1, :])).astype(a_v.dtype)

    half = dim // 2
    positions = jnp.broadcast_to(posv_ref[...].astype(jnp.float32), (dim, rows)).T
    angles = positions * freq_ref[0:1, :]
    cos_all = jnp.cos(angles)
    sin_all = jnp.sin(angles)
    sin_all = jnp.where(lax.broadcasted_iota(jnp.int32, sin_all.shape, 1) < half, -sin_all, sin_all)
    slabs_started = 0
    for n, (kind, _, i) in enumerate(jobs):
        w_copy(n).wait()
        upto = n_slab * (n + 1) // len(jobs)
        for d in range(slabs_started, upto):
            for copy in slab_copies(d):
                copy.start()
        slabs_started = upto
        prod = jnp.dot(a_v[...], w_v[n], preferred_element_type=jnp.float32)
        for h in range(chunk // dim):
            val = prod[:, h * dim:(h + 1) * dim]
            if kind != 'v':
                val = val * cos_all + pltpu.roll(val, half, 1) * sin_all
            head = i * (chunk // dim) + h
            if kind == 'q':
                q_s[pl.ds(head, rows, stride=heads), :] = val
            else:
                for r in range(window // kv_heads):
                    (kn_s if kind == 'k' else vn_s)[pl.ds(r * kv_heads + head, rows, stride=window), :] = val

    col = lax.broadcasted_iota(jnp.int32, (heads, span), 1)
    row = lax.broadcasted_iota(jnp.int32, (heads, span), 0)
    same_head = col % kv_heads == row // group
    lane = lax.broadcasted_iota(jnp.int32, (heads, dim), 1)
    win_time = lax.broadcasted_iota(jnp.int32, (window, dim), 0) // kv_heads
    per_window = window // kv_heads

    @pl.loop(0, n_slab)
    def _(d):
        for copy in slab_copies(d):
            copy.wait()
        last = []
        for j in range(row_block):
            b = d * row_block + j
            here = pos_ref[0, b] - first_pos
            last.append(here)
            slot = jnp.clip(here, 0, seq_block - 1)
            at = pl.ds(pl.multiple_of(slot // per_window * window, window), window)
            hit = win_time == jnp.where(here == slot, slot % per_window, -1)
            new = pl.ds(pl.multiple_of(b * window, window), window)
            ko_ref[b, at, :] = jnp.where(hit, kn_s[new, :], ko_ref[b, at, :].astype(jnp.float32)).astype(ko_ref.dtype)
            vo_ref[b, at, :] = jnp.where(hit, vn_s[new, :], vo_ref[b, at, :].astype(jnp.float32)).astype(vo_ref.dtype)
        for copy in out_copies(d):
            copy.start()
        scores = []
        for j in range(row_block):
            b = d * row_block + j
            q_b = q_s[pl.ds(pl.multiple_of(b * heads, heads), heads), :].astype(jnp.bfloat16)
            scores.append(lax.dot_general(q_b, ko_ref[b], (((1,), (1,)), ((), ())), preferred_element_type=jnp.float32))
        tops = jnp.zeros((heads, dim), jnp.float32)
        sums = jnp.zeros((heads, dim), jnp.float32)
        weights = []
        for j in range(row_block):
            valid = same_head & (col < (last[j] + 1) * kv_heads)
            capped = jnp.where(valid, SOFT_CAP * jnp.tanh(scores[j] * (dim ** -0.5 / SOFT_CAP)), NEG_FILL)
            top = jnp.max(capped, axis=1, keepdims=True)
            exp_w = jnp.where(valid, jnp.exp(capped - top), 0.0)
            tops = jnp.where(lane == j, top, tops)
            sums = jnp.where(lane == j, jnp.sum(exp_w, axis=1, keepdims=True), sums)
            weights.append(exp_w.astype(jnp.bfloat16))
        slab = d % 2 * (n_slab // 2) + d // 2
        for j in range(row_block):
            b = d * row_block + j
            pack_ref[slab, pl.ds(j * heads, heads), :] = jnp.dot(weights[j], vo_ref[b], preferred_element_type=jnp.float32)
        pack_ref[slab, pl.ds(row_block * heads, heads), :] = tops
        pack_ref[slab, pl.ds((row_block + 1) * heads, heads), :] = sums

    for d in range(n_slab):
        for copy in out_copies(d):
            copy.wait()


def in_hbm(operand):
    return pltpu.with_memory_space_constraint(operand, pltpu.HBM)


def attend(x_in, cur_pos, w_pre, w_q, w_k, w_v, k_cache, v_cache, n_sp):
    rows, seq_block, kv_heads, dim = k_cache.shape
    width = x_in.shape[1]
    heads = w_q.shape[1] // dim
    chunk = 2 * dim
    window = 16
    n_jobs = (w_q.shape[1] + w_k.shape[1] + w_v.shape[1]) // chunk
    inv_freq = ROPE_BASE ** (-2.0 * jnp.arange(dim // 2, dtype=jnp.float32) / dim)
    freq = jnp.broadcast_to(jnp.concatenate([inv_freq, inv_freq])[None], (8, dim))
    flat = (rows, seq_block * kv_heads, dim)
    sems = pltpu.SemaphoreType.DMA
    vmem = pl.BlockSpec(memory_space=pltpu.VMEM)
    hbm = pl.BlockSpec(memory_space=pltpu.HBM)
    pack, k_out, v_out = pl.pallas_call(
        functools.partial(attend_kernel, kv_heads),
        out_shape=(jax.ShapeDtypeStruct((n_sp, rows // n_sp * heads + 2 * heads, dim), jnp.float32),
                   jax.ShapeDtypeStruct(flat, k_cache.dtype), jax.ShapeDtypeStruct(flat, v_cache.dtype)),
        in_specs=[vmem] + [hbm] * 8,
        out_specs=(vmem, hbm, hbm),
        scratch_shapes=[
            pltpu.SMEM((1, rows), cur_pos.dtype),
            pltpu.VMEM((1, rows), cur_pos.dtype),
            pltpu.VMEM((rows, width), x_in.dtype),
            pltpu.VMEM((width // dim, dim), jnp.float32),
            pltpu.VMEM((rows, width), jnp.bfloat16),
            pltpu.VMEM((n_jobs, width, chunk), w_q.dtype),
            pltpu.VMEM(((rows + 1) * heads, dim), jnp.float32),
            pltpu.VMEM(((rows + 1) * window, dim), jnp.float32),
            pltpu.VMEM(((rows + 1) * window, dim), jnp.float32),
            pltpu.VMEM(flat, k_cache.dtype),
            pltpu.VMEM(flat, v_cache.dtype),
            sems((4,)), sems((n_jobs,)), sems((n_sp,)), sems((n_sp,)), sems((n_sp,)), sems((n_sp,)),
        ],
        compiler_params=pltpu.CompilerParams(vmem_limit_bytes=48 * 2**20),
        cost_estimate=pl.CostEstimate(flops=2 * rows * w_q.size * 2, bytes_accessed=w_q.size * 4 + k_cache.size * 4, transcendentals=0),
        name='attend',
    )(freq, in_hbm(cur_pos[None]), in_hbm(x_in), in_hbm(w_pre.reshape(-1, dim)),
      in_hbm(w_q), in_hbm(w_k), in_hbm(w_v), in_hbm(k_cache.reshape(flat)), in_hbm(v_cache.reshape(flat)))
    return pack, k_out.reshape(k_cache.shape), v_out.reshape(v_cache.shape)


def finish(o_pack, w_o, x_in, w_post, heads):
    rows, width = x_in.shape
    _, slab_rows, dim = o_pack.shape
    row_block = rows // (2 * RING)
    n_chunk = 3 if width % (3 * 256) == 0 else 1
    sems = pltpu.SemaphoreType.DMA
    vmem = pl.BlockSpec(memory_space=pltpu.VMEM)
    hbm = pl.BlockSpec(memory_space=pltpu.HBM)
    return pl.pallas_call(
        functools.partial(comm_kernel, heads),
        out_shape=jax.ShapeDtypeStruct((rows, width), x_in.dtype),
        in_specs=[vmem, hbm, hbm, hbm],
        out_specs=vmem,
        scratch_shapes=[
            pltpu.VMEM(w_o.shape, w_o.dtype),
            pltpu.VMEM((row_block, width), x_in.dtype),
            pltpu.VMEM((width // dim, dim), jnp.float32),
            pltpu.VMEM((RING, slab_rows, dim), jnp.float32),
            pltpu.VMEM((RING, slab_rows, dim), jnp.float32),
            pltpu.VMEM((RING - 1, slab_rows, dim), jnp.float32),
            pltpu.VMEM(((row_block + 1) * heads, dim), jnp.float32),
            pltpu.VMEM((RING, row_block // RING, width), jnp.float32),
            pltpu.VMEM((RING - 1, row_block // RING, width), jnp.float32),
            pltpu.VMEM((2 * RING * RING, row_block // RING, width), jnp.float32),
            sems((RING,)), sems((2,)),
            sems((RING,)), sems((RING,)),
            sems((RING - 1,)), sems((RING - 1,)),
            sems((n_chunk * (RING - 1),)), sems((n_chunk * (RING - 1),)),
            sems((N_GATHER,)), sems((N_GATHER,)),
            sems((RING * RING,)), sems((RING * RING,)),
        ],
        compiler_params=pltpu.CompilerParams(collective_id=0, has_side_effects=True, vmem_limit_bytes=22 * 2**20),
        cost_estimate=pl.CostEstimate(flops=2 * rows * w_o.size // 8, bytes_accessed=w_o.size * 2, transcendentals=0),
        name='finish',
    )(o_pack, in_hbm(w_o), in_hbm(x_in), in_hbm(w_post.reshape(-1, dim)))


def solution(mesh):
    cache_spec = P('dp', 'sp', 'tp', None)
    n_sp = mesh.shape['sp']
    assert n_sp == 2 * RING and mesh.shape['tp'] == RING

    def local_step(x_in, cur_pos, w_pre, w_q, w_k, w_v, w_o, w_post, k_cache, v_cache):
        heads_local = w_q.shape[1] // k_cache.shape[3]
        slabs, k_out, v_out = attend(x_in, cur_pos, w_pre, w_q, w_k, w_v, k_cache, v_cache, n_sp)
        x_out = finish(slabs, w_o, x_in, w_post, heads_local)
        return x_out, k_out, v_out

    return jax.shard_map(local_step, mesh=mesh,
                         in_specs=(P('dp', None), P('dp'), P(None), P(None, 'tp'), P(None, 'tp'), P(None, 'tp'), P('tp', None), P(None), cache_spec, cache_spec),
                         out_specs=(P('dp', None), cache_spec, cache_spec), check_vma=False)
```
